128 devices in a mesh: gx: 128 (over z, y, x, core).
Axes of the slice: x: 4, y: 4, z: 4, core: 2. Of those that a mesh axis runs over, the one named last changes fastest.
Arguments:
- value: float32 [256, 48, 32, 128], P('gx'), may hold values from -6 to 6
- target: float32 [256, 48, 32, 128], P('gx'), may hold values from -6 to 6
- obstacle: float32 [256, 48, 32, 128], P('gx'), may hold values from -6 to -0.5
- fractions: float32 [16, 4], replicated, may hold values from 0 to 1
- control_cost: float32 [16], replicated, may hold values from 0 to 0.5
- shard_offset: int32 [16], replicated, may hold values from -8 to 8, as said below
- cell_offset: int32 [16], replicated, may hold values from 0 to 1
- grid_offset: int32 [16, 3], replicated, may hold values from -4 to 4
Outputs:
- updated: float32 [256, 48, 32, 128], P('gx')
The draws below stay inside these ranges and needn't reach their ends.
Inputs may be any that keep to these rules, and one draw needn't show every extreme that they name: `shard_offset`: every draw holds both -8 and 8.
All inputs are finite; a program needn't handle non-finite values.
Results may differ from the reference program's by a relative error of at most 0.00002.
Values sent between devices are 32-bit elements; how exact they have to be, the bound alone decides.
A program may use at most 128 MiB of HBM per device.

```python
import jax
import jax.numpy as jnp
from jax import lax

CX = 2
NY = 48
NZ = 32
NW = 128
NCTRL = 16
REACH = 8
NX = 256


def draw_shard_offset(key, part):
    first_key, second_key = jax.random.split(jax.random.fold_in(key, 11))
    offsets = jax.random.randint(first_key, (NCTRL,), -REACH, REACH + 1)
    order = jax.random.permutation(second_key, NCTRL)
    offsets = offsets.at[order[0]].set(-REACH).at[order[1]].set(REACH)
    return offsets.astype(jnp.int32)


def set_ends(entries, own_key, smallest, top_value):
    index_at = [jax.random.randint(jax.random.fold_in(own_key, axis), (), 0, length) for axis, length in enumerate(entries.shape)]
    widest = entries.shape.index(max(entries.shape))
    neighbour = index_at[:widest] + [(index_at[widest] + 1) % entries.shape[widest]] + index_at[widest + 1:]
    return entries.at[tuple(index_at)].set(smallest).at[tuple(neighbour)].set(top_value)


def block_levels(own_key, shape, cuts, low, high):
    def one(axis_at, blocks):
        heights = jax.random.uniform(jax.random.fold_in(jax.random.fold_in(own_key, 6), axis_at), (blocks,), jnp.float32, low / len(cuts), high / len(cuts))
        return jnp.repeat(jnp.exp(heights), shape[axis_at] // blocks).reshape((-1,) + (1,) * (len(shape) - axis_at - 1))

    level = one(*cuts[0])
    for cut in cuts[1:]:
        level = level * one(*cut)
    return level


def bell_draw(own_key, extent, width, reach, cuts=(), held_as=jnp.bfloat16):
    gain = block_levels(own_key, extent, cuts, -0.22, 0.18) if cuts else 1.0
    array = jax.random.normal(own_key, extent, jnp.float32) * width * gain
    return jnp.minimum(jnp.maximum(array, -reach), reach).astype(held_as)


def setup_inputs(seed: int = 0) -> dict:
    arg_keys = jax.random.split(jax.random.key(seed), 9)
    value = bell_draw(arg_keys[0], (NX, NY, NZ, NW), 1.0, 6.0, ((0, 128),), jnp.float32)
    target = bell_draw(arg_keys[1], (NX, NY, NZ, NW), 1.0, 6.0, ((0, 128),), jnp.float32)
    obstacle = jnp.clip(-6.0 + 5.5 * jax.random.uniform(arg_keys[2], (NX, NY, NZ, NW), jnp.float32) ** block_levels(arg_keys[2], (NX, NY, NZ, NW), ((0, 128),), -0.2, 0.2), -6.0, -0.5)
    fractions = jnp.clip(jax.random.uniform(arg_keys[3], (NCTRL, 4), jnp.float32, 0.0, 1.0), 0.0, 1.0)
    control_cost = jnp.clip(jax.random.uniform(arg_keys[4], (NCTRL,), jnp.float32, 0.0, 0.5), 0.0, 0.5)
    shard_offset = draw_shard_offset(jax.random.fold_in(arg_keys[8], 71), 0)
    cell_offset = set_ends(jax.random.randint(arg_keys[6], (NCTRL,), 0, CX), jax.random.fold_in(arg_keys[6], 1), 0, CX - 1).astype(jnp.int32)
    grid_offset = set_ends(jax.random.randint(arg_keys[7], (NCTRL, 3), -4, 5), jax.random.fold_in(arg_keys[7], 1), -4, 4).astype(jnp.int32)
    return {"value": value, "target": target, "obstacle": obstacle, "fractions": fractions, "control_cost": control_cost, "shard_offset": shard_offset, "cell_offset": cell_offset, "grid_offset": grid_offset}


def blend(low, high, frac):
    return (1.0 - frac) * low + frac * high


def reference(value, target, obstacle, fractions, control_cost, shard_offset, cell_offset, grid_offset):
    def one_control(u, best):
        along = (shard_offset[u] * CX + cell_offset[u]).astype(jnp.int32)
        field = blend(jnp.roll(value, -along, axis=0), jnp.roll(value, -along - 1, axis=0), fractions[u, 0])
        for axis_k in range(1, 4):
            moved = grid_offset[u, axis_k - 1].astype(jnp.int32)
            field = blend(jnp.roll(field, -moved, axis=axis_k), jnp.roll(field, -moved - 1, axis=axis_k), fractions[u, axis_k])
        return jnp.minimum(best, field + control_cost[u])

    start = jnp.full(value.shape, jnp.inf, jnp.float32)
    best = lax.fori_loop(0, NCTRL, one_control, start)
    return jnp.maximum(obstacle, jnp.minimum(target, best))
```

```python
import functools

import jax
import jax.numpy as jnp
from jax import lax
from jax.experimental import pallas as pl
from jax.experimental.pallas import tpu as pltpu
from jax.sharding import PartitionSpec as P

CX, NY, NZ, NW, NCTRL = 2, 48, 32, 128, 16
ROW = 8
RX = ROW * CX
LO, HI = 4, 5
ENDS = (17, 29, 41, 48)
STAGES = len(ENDS)
CUTS = (0,) + ENDS
OUTS = (0,) + tuple(e - LO - HI for e in ENDS[:-1]) + (NY,)
G, ZT = 4, 2
MESH = pl.DeviceIdType.MESH
(RIGHT, LEFT, FWD_R, FWD_L, D_OWN, D_L, D_R, D_O0, D_O1, HALO, D_HALO, HALO2, UP, DOWN) = range(14)
KINDS = 14


def kernel(frac, cost, so, co, go, value, target, obstacle, out,
           B, C, P1, Pm, Q1, Qm, A, T, O, ip, fp, ssem, rsem, lsem):
    n = lax.axis_size("gx")
    me = lax.axis_index("gx")
    j = lax.rem(me, ROW)
    base = me - j
    core = lax.rem(j, 2)
    jr, jl, jo, jp = lax.rem(j + 2, ROW), lax.rem(j + 6, ROW), lax.rem(j + 4, ROW), j + 1 - 2 * core
    qr, ql, qo = jr + 1 - 2 * core, jl + 1 - 2 * core, jo + 1 - 2 * core
    right, left, mate = base + jr, base + jl, base + jp
    up, down = lax.rem(me + ROW, n), lax.rem(me + n - ROW, n)
    last = j == ROW - 1

    loads = [pltpu.make_async_copy(value, B.at[j], lsem.at[0]),
             pltpu.make_async_copy(target, T, lsem.at[1]),
             pltpu.make_async_copy(obstacle, O, lsem.at[2])]
    loads[0].start()

    barrier = pltpu.get_barrier_semaphore()
    for peer in (right, left, mate, up, down):
        pl.semaphore_signal(barrier, inc=1, device_id=(peer,), device_id_type=MESH)

    def params(u, _):
        off = 2 * so[u] + co[u]
        for i in range(2):
            q = 2 * j + i + off
            d = jnp.where(q < 0, -1, jnp.where(q < RX, 0, 1))
            ip[i * NCTRL + u] = q - RX * d
            for e, which in enumerate((0, 1, -1)):
                fp[(8 + 3 * i + e) * NCTRL + u] = jnp.where(d == which, cost[u], jnp.inf)
        ip[2 * NCTRL + u] = go[u, 0]
        ip[3 * NCTRL + u] = go[u, 1] + 8
        ip[4 * NCTRL + u] = (NW - go[u, 2]) & (NW - 1)
        ip[5 * NCTRL + u] = (NW - 1 - go[u, 2]) & (NW - 1)
        f0, f1, f2, f3 = frac[u, 0], frac[u, 1], frac[u, 2], frac[u, 3]
        fp[u] = (1.0 - f0) * (1.0 - f2)
        fp[NCTRL + u] = (1.0 - f0) * f2
        fp[2 * NCTRL + u] = f0 * (1.0 - f2)
        fp[3 * NCTRL + u] = f0 * f2
        fp[4 * NCTRL + u] = 1.0 - f1
        fp[5 * NCTRL + u] = f1
        fp[6 * NCTRL + u] = 1.0 - f3
        fp[7 * NCTRL + u] = f3
        return 0

    lax.fori_loop(0, NCTRL, params, 0)
    loads[0].wait()
    pl.semaphore_wait(barrier, 5)

    def remote(kind, k, src, dst, peer):
        return pltpu.make_async_remote_copy(src_ref=src, dst_ref=dst, send_sem=ssem.at[kind, k],
                                            recv_sem=rsem.at[kind, k], device_id=(peer,), device_id_type=MESH)

    def block(slab, k, row=None):
        ys = pl.ds(CUTS[k], CUTS[k + 1] - CUTS[k])
        return B.at[slab, :, ys] if row is None else B.at[slab, row, ys]

    def same(kind, k, peer, slab, row=None):
        return remote(kind, k, block(slab, k, row), block(slab, k, row), peer)

    def send(kind, k):
        return {
            RIGHT: lambda: same(kind, k, right, j),
            LEFT: lambda: same(kind, k, left, j),
            FWD_R: lambda: same(kind, k, right, jl, 0),
            FWD_L: lambda: same(kind, k, left, jr, 1),
            D_OWN: lambda: same(kind, k, mate, j),
            D_L: lambda: same(kind, k, mate, jl),
            D_R: lambda: same(kind, k, mate, jr),
            D_O0: lambda: same(kind, k, mate, jo, 0),
            D_O1: lambda: same(kind, k, mate, jo, 1),
            HALO: lambda: remote(kind, k, block(0, k, 0), block(ROW, k, 0), down),
            D_HALO: lambda: same(kind, k, mate, ROW, 0),
            HALO2: lambda: remote(kind, k, block(0, k, 1), block(ROW, k, 1), down),
        }[kind]()

    def recv(kind, k):
        return {
            RIGHT: lambda: same(kind, k, right, jl),
            LEFT: lambda: same(kind, k, left, jr),
            FWD_R: lambda: same(kind, k, right, jo, 0),
            FWD_L: lambda: same(kind, k, left, jo, 1),
            D_OWN: lambda: same(kind, k, mate, jp),
            D_L: lambda: same(kind, k, mate, ql),
            D_R: lambda: same(kind, k, mate, qr),
            D_O0: lambda: same(kind, k, mate, qo, 0),
            D_O1: lambda: same(kind, k, mate, qo, 1),
            HALO: lambda: same(kind, k, down, ROW, 0),
            D_HALO: lambda: same(kind, k, mate, ROW, 0),
            HALO2: lambda: same(kind, k, down, ROW, 1),
        }[kind]()

    def partial(kind, k):
        ys = pl.ds(OUTS[k], OUTS[k + 1] - OUTS[k])
        src, dst, peer = (Pm, Qm, up) if kind == UP else (P1, Q1, down)
        return remote(kind, k, src.at[:, ys], dst.at[:, ys], peer)

    def fill(k):
        lo, hi = CUTS[k], CUTS[k + 1]

        def put(row, src, y, to):
            C[row, to, pl.ds(0, 8), :] = src[pl.ds(24, 8), :]
            C[row, to, pl.ds(8, 32), :] = src[...]
            C[row, to, pl.ds(40, 8), :] = src[pl.ds(0, 8), :]

        def one(shift, row2):
            def step(y, _):
                rows = (RX + 1,) if row2 else range(RX + 1)
                for row in rows:
                    put(row, B.at[row // 2, row % 2, y], y, y + shift)
                return 0
            return step

        lax.fori_loop(lo, hi, one(0, False), 0)
        if k == 0:
            lax.fori_loop(0, LO + HI, one(NY, False), 0)

        @pl.when(last)
        def _():
            lax.fori_loop(lo, hi, one(0, True), 0)
            if k == 0:
                lax.fori_loop(0, LO + HI, one(NY, True), 0)

    def compute(k):
        lo, hi = OUTS[k], OUTS[k + 1]

        def tile(t, _):
            i = lax.rem(t, 2)
            t = lax.div(t, 2)
            z = lax.rem(t, NZ // (8 * ZT)) * (8 * ZT)
            y = lo + lax.div(t, NZ // (8 * ZT)) * G

            def control(u, acc):
                row = ip[i * NCTRL + u]
                yy = y + LO + ip[2 * NCTRL + u]
                zz = z + ip[3 * NCTRL + u]
                s1, s2 = ip[4 * NCTRL + u], ip[5 * NCTRL + u]
                f = [fp[q * NCTRL + u] for q in range(8)]
                c = [fp[(8 + 3 * i + e) * NCTRL + u] for e in range(3)]
                fields = []
                for q in range(G + 1):
                    low = f[0] * C[row, yy + q, pl.ds(zz, 8 * ZT), :] + f[1] * C[row, yy + q, pl.ds(zz + 1, 8 * ZT), :]
                    high = f[2] * C[row + 1, yy + q, pl.ds(zz, 8 * ZT), :] + f[3] * C[row + 1, yy + q, pl.ds(zz + 1, 8 * ZT), :]
                    fields.append(low + high)
                new = []
                for q in range(G):
                    h = f[4] * fields[q] + f[5] * fields[q + 1]
                    w = f[6] * pltpu.roll(h, s1, 1) + f[7] * pltpu.roll(h, s2, 1)
                    new += [jnp.minimum(acc[3 * q + e], w + c[e]) for e in range(3)]
                return tuple(new)

            start = tuple([jnp.full((8 * ZT, NW), jnp.inf, jnp.float32)] * (3 * G))
            acc = lax.fori_loop(0, NCTRL, control, start, unroll=True)
            zs = pl.ds(pl.multiple_of(z, 8), 8 * ZT)
            for q in range(G):
                for e, ref in enumerate((A, P1, Pm)):
                    ref[i, y + q, zs, :] = acc[3 * q + e]
            return 0

        lax.fori_loop(0, 2 * ((hi - lo) // G) * (NZ // (8 * ZT)), tile, 0)

    def combine(k):
        partial(UP, k).wait_recv()
        partial(DOWN, k).wait_recv()
        lo, hi = OUTS[k], OUTS[k + 1]

        def step(y, _):
            at = lax.rem(y + LO, NY)
            for i in range(2):
                best = jnp.minimum(A[i, y], jnp.minimum(Q1[i, y], Qm[i, y]))
                A[i, y] = jnp.maximum(O[i, at], jnp.minimum(T[i, at], best))
            return 0

        lax.fori_loop(lo, hi, step, 0)

    for k in range(min(2, STAGES)):
        send(RIGHT, k).start()
        send(LEFT, k).start()
    for k in range(STAGES):
        send(D_OWN, k).start()
    loads[1].start()
    loads[2].start()
    for k in range(STAGES):
        recv(RIGHT, k).wait_recv()
        send(FWD_R, k).start()
        send(D_L, k).start()
        recv(LEFT, k).wait_recv()
        send(FWD_L, k).start()
        send(D_R, k).start()
        if k + 2 < STAGES:
            send(RIGHT, k + 2).start()
            send(LEFT, k + 2).start()
        recv(FWD_R, k).wait_recv()
        send(D_O0, k).start()
        recv(FWD_L, k).wait_recv()
        send(D_O1, k).start()
        for kind in (D_OWN, D_L, D_R, D_O0, D_O1):
            recv(kind, k).wait_recv()

        @pl.when(core == 0)
        def _():
            send(HALO, k).start()

        @pl.when(last)
        def _():
            send(HALO2, k).start()

        @pl.when(core == 0)
        def _():
            recv(HALO, k).wait_recv()
            send(D_HALO, k).start()

        @pl.when(last)
        def _():
            recv(HALO2, k).wait_recv()

        @pl.when(core == 1)
        def _():
            recv(D_HALO, k).wait_recv()

        fill(k)
        compute(k)
        partial(UP, k).start()
        partial(DOWN, k).start()
        if k == 0:
            loads[1].wait()
            loads[2].wait()
        else:
            combine(k - 1)
    combine(STAGES - 1)

    stores = [pltpu.make_async_copy(A.at[:, pl.ds(0, NY - LO)], out.at[:, pl.ds(LO, NY - LO)], lsem.at[3]),
              pltpu.make_async_copy(A.at[:, pl.ds(NY - LO, LO)], out.at[:, pl.ds(0, LO)], lsem.at[4])]
    for copy in stores:
        copy.start()
    for k in range(STAGES):
        for kind in (RIGHT, LEFT, FWD_R, FWD_L, D_OWN, D_L, D_R, D_O0, D_O1):
            send(kind, k).wait_send()
        partial(UP, k).wait_send()
        partial(DOWN, k).wait_send()

        @pl.when(core == 0)
        def _():
            send(HALO, k).wait_send()
            send(D_HALO, k).wait_send()

        @pl.when(last)
        def _():
            send(HALO2, k).wait_send()

    for copy in stores:
        copy.wait()


def body(value, target, obstacle, fractions, control_cost, shard_offset, cell_offset, grid_offset):
    slab = (CX, NY, NZ, NW)
    vmem = functools.partial(pltpu.VMEM, dtype=jnp.float32)
    smem = pl.BlockSpec(memory_space=pltpu.SMEM)
    anywhere = pl.BlockSpec(memory_space=pl.ANY)
    return pl.pallas_call(
        kernel,
        name="reach_avoid",
        out_shape=jax.ShapeDtypeStruct(slab, jnp.float32),
        in_specs=[smem] * 5 + [anywhere] * 3,
        out_specs=anywhere,
        scratch_shapes=[
            vmem((ROW + 1,) + slab),
            vmem((RX + 2, NY + LO + HI, NZ + 16, NW)),
            vmem(slab), vmem(slab), vmem(slab), vmem(slab), vmem(slab), vmem(slab), vmem(slab),
            pltpu.SMEM((6 * NCTRL,), jnp.int32),
            pltpu.SMEM((14 * NCTRL,), jnp.float32),
            pltpu.SemaphoreType.DMA((KINDS, STAGES)),
            pltpu.SemaphoreType.DMA((KINDS, STAGES)),
            pltpu.SemaphoreType.DMA((5,)),
        ],
        compiler_params=pltpu.CompilerParams(collective_id=0, has_side_effects=True, vmem_limit_bytes=62 << 20),
    )(fractions, control_cost, shard_offset, cell_offset, grid_offset, value, target, obstacle)


def solution(mesh):
    grid = P("gx", None, None, None)
    return jax.shard_map(body, mesh=mesh, in_specs=(grid, grid, grid, P(), P(), P(), P(), P()), out_specs=grid,
                         check_vma=False)
```

```python
import functools

import jax
import jax.numpy as jnp
from jax import lax
from jax.experimental import pallas as pl
from jax.experimental.pallas import tpu as pltpu
from jax.sharding import PartitionSpec as P

CX, NY, NZ, NW, NCTRL = 2, 48, 32, 128, 16
ROW = 8
RX = ROW * CX
LO, HI = 4, 5
ENDS = (13, 17, 21, 25, 29, 33, 37, 41, 45, 48)
ORDER = tuple(zip("NNONOWNOWNOWNOWNOWNOWNONWOOWWW", (0, 1, 0, 2, 1, 0, 3, 2, 1, 4, 3, 2, 5, 4, 3, 6, 5, 4, 7, 6, 5, 8, 7, 9, 6, 8, 9, 7, 8, 9)))
DEPTH = 2
STAGES = len(ENDS)
CUTS = (0,) + ENDS
OUTS = (0,) + tuple(e - LO - HI for e in ENDS[:-1]) + (NY,)
G, ZT = 4, 2
PARTS = tuple((k, lo, OUTS[k + 1]) for k, lo in enumerate(OUTS[:-2])) + tuple(
    (STAGES - 1, lo, lo + G) for lo in range(OUTS[-2], NY, G))
MESH = pl.DeviceIdType.MESH
(RIGHT, LEFT, FWD_R, FWD_L, D_OWN, D_L, D_R, D_O0, D_O1, HALO, HALO_B, HALO2) = range(12)
KINDS = 12


def kernel(frac, cost, so, co, go, value, target, obstacle, out,
           B, C, P1, Pm, Q1, Qm, A, T, O, ip, fp, ssem, rsem, psem, qsem, osem, lsem):
    n = lax.axis_size("gx")
    me = lax.axis_index("gx")
    j = lax.rem(me, ROW)
    base = me - j
    core = lax.rem(j, 2)
    jr, jl, jo, jp = lax.rem(j + 2, ROW), lax.rem(j + 6, ROW), lax.rem(j + 4, ROW), j + 1 - 2 * core
    qr, ql, qo = jr + 1 - 2 * core, jl + 1 - 2 * core, jo + 1 - 2 * core
    right, left, mate = base + jr, base + jl, base + jp
    up, down = lax.rem(me + ROW, n), lax.rem(me + n - ROW, n)
    beyond = jnp.where(core == 0, down + 1, up - 1)
    last = j == ROW - 1
    beside_last = j == ROW - 2

    loads = [pltpu.make_async_copy(value, B.at[j], lsem.at[0]),
             pltpu.make_async_copy(target, T, lsem.at[1]),
             pltpu.make_async_copy(obstacle, O, lsem.at[2])]
    loads[0].start()

    barrier = pltpu.get_barrier_semaphore()
    for peer in (right, left, mate, up, down, beyond):
        pl.semaphore_signal(barrier, inc=1, device_id=(peer,), device_id_type=MESH)

    def params(u, _):
        off = 2 * so[u] + co[u]
        for i in range(2):
            q = 2 * j + i + off
            d = jnp.where(q < 0, -1, jnp.where(q < RX, 0, 1))
            ip[i * NCTRL + u] = q - RX * d
            for e, which in enumerate((0, 1, -1)):
                fp[(8 + 3 * i + e) * NCTRL + u] = jnp.where(d == which, cost[u], jnp.inf)
        ip[2 * NCTRL + u] = go[0, u]
        ip[3 * NCTRL + u] = go[1, u] + 8
        ip[4 * NCTRL + u] = (NW - go[2, u]) & (NW - 1)
        ip[5 * NCTRL + u] = (NW - 1 - go[2, u]) & (NW - 1)
        f0, f1, f2, f3 = frac[0, u], frac[1, u], frac[2, u], frac[3, u]
        fp[u] = (1.0 - f0) * (1.0 - f2)
        fp[NCTRL + u] = (1.0 - f0) * f2
        fp[2 * NCTRL + u] = f0 * (1.0 - f2)
        fp[3 * NCTRL + u] = f0 * f2
        fp[4 * NCTRL + u] = 1.0 - f1
        fp[5 * NCTRL + u] = f1
        fp[6 * NCTRL + u] = 1.0 - f3
        fp[7 * NCTRL + u] = f3
        return 0

    lax.fori_loop(0, NCTRL, params, 0)
    loads[0].wait()
    pl.semaphore_wait(barrier, 6)

    def remote(kind, k, src, dst, peer):
        return pltpu.make_async_remote_copy(src_ref=src, dst_ref=dst, send_sem=ssem.at[kind, k],
                                            recv_sem=rsem.at[kind, k], device_id=(peer,), device_id_type=MESH)

    def block(slab, k, row=None):
        ys = pl.ds(CUTS[k], CUTS[k + 1] - CUTS[k])
        return B.at[slab, :, ys] if row is None else B.at[slab, row, ys]

    def same(kind, k, peer, slab, row=None):
        return remote(kind, k, block(slab, k, row), block(slab, k, row), peer)

    def send(kind, k):
        return {
            RIGHT: lambda: same(kind, k, right, j),
            LEFT: lambda: same(kind, k, left, j),
            FWD_R: lambda: same(kind, k, right, jl, 0),
            FWD_L: lambda: same(kind, k, left, jr, 1),
            D_OWN: lambda: remote(kind, k, B.at[j], B.at[j], mate),
            D_L: lambda: same(kind, k, mate, jl),
            D_R: lambda: same(kind, k, mate, jr),
            D_O0: lambda: same(kind, k, mate, jo, 0),
            D_O1: lambda: same(kind, k, mate, jo, 1),
            HALO: lambda: remote(kind, k, block(0, k, 0), block(ROW, k, 0), down),
            HALO_B: lambda: remote(kind, k, block(0, k, 0), block(ROW, k, 0), beyond),
            HALO2: lambda: remote(kind, k, block(0, k, 1), block(ROW, k, 1), beyond),
        }[kind]()

    def recv(kind, k):
        return {
            RIGHT: lambda: same(kind, k, right, jl),
            LEFT: lambda: same(kind, k, left, jr),
            FWD_R: lambda: same(kind, k, right, jo, 0),
            FWD_L: lambda: same(kind, k, left, jo, 1),
            D_OWN: lambda: remote(kind, k, B.at[jp], B.at[jp], mate),
            D_L: lambda: same(kind, k, mate, ql),
            D_R: lambda: same(kind, k, mate, qr),
            D_O0: lambda: same(kind, k, mate, qo, 0),
            D_O1: lambda: same(kind, k, mate, qo, 1),
            HALO: lambda: same(kind, k, down, ROW, 0),
            HALO_B: lambda: same(kind, k, beyond, ROW, 0),
            HALO2: lambda: same(kind, k, beyond, ROW, 1),
        }[kind]()

    def partial(kind, part):
        ys = pl.ds(PARTS[part][1], PARTS[part][2] - PARTS[part][1])
        src, dst, peer = (Pm, Qm, up) if kind == 0 else (P1, Q1, down)
        return pltpu.make_async_remote_copy(src_ref=src.at[:, ys], dst_ref=dst.at[:, ys], send_sem=psem.at[kind, part],
                                            recv_sem=qsem.at[kind, part], device_id=(peer,), device_id_type=MESH)

    def fill(k):
        lo, hi = CUTS[k], CUTS[k + 1]

        def put(row, src, y, to):
            C[row, to, pl.ds(0, 8), :] = src[pl.ds(24, 8), :]
            C[row, to, pl.ds(8, 32), :] = src[...]
            C[row, to, pl.ds(40, 8), :] = src[pl.ds(0, 8), :]

        def one(shift, row2):
            def step(y, _):
                rows = (RX + 1,) if row2 else range(RX + 1)
                for row in rows:
                    put(row, B.at[row // 2, row % 2, y], y, y + shift)
                return 0
            return step

        lax.fori_loop(lo, hi, one(0, False), 0)
        if k == 0:
            lax.fori_loop(0, LO + HI, one(NY, False), 0)

        @pl.when(last)
        def _():
            lax.fori_loop(lo, hi, one(0, True), 0)
            if k == 0:
                lax.fori_loop(0, LO + HI, one(NY, True), 0)

    def compute(part):
        _, lo, hi = PARTS[part]

        def tile(t, _):
            i = lax.rem(t, 2)
            t = lax.div(t, 2)
            z = lax.rem(t, NZ // (8 * ZT)) * (8 * ZT)
            y = lo + lax.div(t, NZ // (8 * ZT)) * G

            def control(u, acc):
                row = ip[i * NCTRL + u]
                yy = y + LO + ip[2 * NCTRL + u]
                zz = z + ip[3 * NCTRL + u]
                s1, s2 = ip[4 * NCTRL + u], ip[5 * NCTRL + u]
                f = [fp[q * NCTRL + u] for q in range(8)]
                c = [fp[(8 + 3 * i + e) * NCTRL + u] for e in range(3)]
                fields = []
                for q in range(G + 1):
                    low = f[0] * C[row, yy + q, pl.ds(zz, 8 * ZT), :] + f[1] * C[row, yy + q, pl.ds(zz + 1, 8 * ZT), :]
                    high = f[2] * C[row + 1, yy + q, pl.ds(zz, 8 * ZT), :] + f[3] * C[row + 1, yy + q, pl.ds(zz + 1, 8 * ZT), :]
                    fields.append(low + high)
                new = []
                for q in range(G):
                    h = f[4] * fields[q] + f[5] * fields[q + 1]
                    w = f[6] * pltpu.roll(h, s1, 1) + f[7] * pltpu.roll(h, s2, 1)
                    new += [jnp.minimum(acc[3 * q + e], w + c[e]) for e in range(3)]
                return tuple(new)

            start = tuple([jnp.full((8 * ZT, NW), jnp.inf, jnp.float32)] * (3 * G))
            acc = lax.fori_loop(0, NCTRL, control, start, unroll=True)
            zs = pl.ds(pl.multiple_of(z, 8), 8 * ZT)
            for q in range(G):
                for e, ref in enumerate((A, P1, Pm)):
                    ref[i, y + q, zs, :] = acc[3 * q + e]
            return 0

        lax.fori_loop(0, 2 * ((hi - lo) // G) * (NZ // (8 * ZT)), tile, 0)

    def combine(part):
        partial(0, part).wait_recv()
        partial(1, part).wait_recv()
        _, lo, hi = PARTS[part]

        def step(y, _):
            at = lax.rem(y + LO, NY)
            for i in range(2):
                best = jnp.minimum(A[i, y], jnp.minimum(Q1[i, y], Qm[i, y]))
                A[i, y] = jnp.maximum(O[i, at], jnp.minimum(T[i, at], best))
            return 0

        lax.fori_loop(lo, hi, step, 0)

    def own(k):
        if k < STAGES:
            send(RIGHT, k).start()
            send(LEFT, k).start()

    def halo(k, which):
        @pl.when(which)
        def _():
            send(HALO, k).start()
            send(HALO_B, k).start()

    def neighbours(k):
        recv(RIGHT, k).wait_recv()
        send(FWD_R, k).start()
        send(D_L, k).start()
        halo(k, j == 2)
        recv(LEFT, k).wait_recv()
        send(FWD_L, k).start()
        send(D_R, k).start()
        halo(k, j == 6)

        @pl.when(beside_last)
        def _():
            send(HALO2, k).start()

        own(k + DEPTH)

    def opposite(k):
        recv(FWD_R, k).wait_recv()
        send(D_O0, k).start()
        halo(k, j == 4)
        recv(FWD_L, k).wait_recv()
        send(D_O1, k).start()

    def work(k):
        if k == 0:
            recv(D_OWN, 0).wait_recv()
        for kind in (D_L, D_R, D_O0, D_O1):
            recv(kind, k).wait_recv()

        @pl.when(core == 0)
        def _():
            recv(HALO, k).wait_recv()

        @pl.when(core == 1)
        def _():
            recv(HALO_B, k).wait_recv()

        @pl.when(last)
        def _():
            recv(HALO2, k).wait_recv()

        fill(k)
        for part, (stage, _, _) in enumerate(PARTS):
            if stage == k:
                compute(part)
                partial(0, part).start()
                partial(1, part).start()

    def store(part):
        _, lo, hi = PARTS[part]
        return pltpu.make_async_copy(A.at[:, pl.ds(lo, hi - lo)], out.at[:, pl.ds((lo + LO) % NY, hi - lo)],
                                     osem.at[part])

    def finish(stage):
        for part, (k, _, _) in enumerate(PARTS):
            if k == stage:
                combine(part)
                store(part).start()

    for k in range(DEPTH):
        own(k)
    send(D_OWN, 0).start()
    for k in range(STAGES):
        halo(k, j == 0)
    loads[1].start()
    loads[2].start()
    for what, k in ORDER:
        if what == "N":
            neighbours(k)
        elif what == "O":
            opposite(k)
        else:
            work(k)
            if k == 1:
                loads[1].wait()
                loads[2].wait()
            if k >= 2:
                finish(k - 2)
    finish(STAGES - 2)
    finish(STAGES - 1)

    send(D_OWN, 0).wait_send()
    for k in range(STAGES):
        for kind in (RIGHT, LEFT, FWD_R, FWD_L, D_L, D_R, D_O0, D_O1):
            send(kind, k).wait_send()

        @pl.when(core == 0)
        def _():
            send(HALO, k).wait_send()
            send(HALO_B, k).wait_send()

        @pl.when(beside_last)
        def _():
            send(HALO2, k).wait_send()

    for part in range(len(PARTS)):
        partial(0, part).wait_send()
        partial(1, part).wait_send()
    for part in range(len(PARTS)):
        store(part).wait()


def body(value, target, obstacle, fractions, control_cost, shard_offset, cell_offset, grid_offset):
    slab = (CX, NY, NZ, NW)
    vmem = functools.partial(pltpu.VMEM, dtype=jnp.float32)
    smem = pl.BlockSpec(memory_space=pltpu.SMEM)
    anywhere = pl.BlockSpec(memory_space=pl.ANY)
    return pl.pallas_call(
        kernel,
        name="reach_avoid",
        out_shape=jax.ShapeDtypeStruct(slab, jnp.float32),
        in_specs=[smem] * 5 + [anywhere] * 3,
        out_specs=anywhere,
        scratch_shapes=[
            vmem((ROW + 1,) + slab),
            vmem((RX + 2, NY + LO + HI, NZ + 16, NW)),
            vmem(slab), vmem(slab), vmem(slab), vmem(slab), vmem(slab), vmem(slab), vmem(slab),
            pltpu.SMEM((6 * NCTRL,), jnp.int32),
            pltpu.SMEM((14 * NCTRL,), jnp.float32),
            pltpu.SemaphoreType.DMA((KINDS, STAGES)),
            pltpu.SemaphoreType.DMA((KINDS, STAGES)),
            pltpu.SemaphoreType.DMA((2, len(PARTS))),
            pltpu.SemaphoreType.DMA((2, len(PARTS))),
            pltpu.SemaphoreType.DMA((len(PARTS),)),
            pltpu.SemaphoreType.DMA((3,)),
        ],
        compiler_params=pltpu.CompilerParams(collective_id=0, has_side_effects=True, vmem_limit_bytes=62 << 20),
    )(fractions.T, control_cost, shard_offset, cell_offset, grid_offset.T, value, target, obstacle)


def solution(mesh):
    grid = P("gx", None, None, None)
    return jax.shard_map(body, mesh=mesh, in_specs=(grid, grid, grid, P(), P(), P(), P(), P()), out_specs=grid,
                         check_vma=False)
```

```python
import functools

import jax
import jax.numpy as jnp
from jax import lax
from jax.experimental import pallas as pl
from jax.experimental.pallas import tpu as pltpu
from jax.sharding import PartitionSpec as P

CX, NY, NZ, NW, NCTRL = 2, 48, 32, 128, 16
ROW = 8
RX = ROW * CX
LO, HI = 4, 5
ENDS = (13, 17, 21, 25, 29, 33, 37, 41, 45, 48)
ORDER = tuple(zip("NNONHOWNHOWNHOWNHOWNHOWNHOWNHONWOHOWHHWW", (0, 1, 0, 2, 0, 1, 0, 3, 1, 2, 1, 4, 2, 3, 2, 5, 3, 4, 3, 6, 4, 5, 4, 7, 5, 6, 5, 8, 6, 7, 9, 6, 8, 7, 9, 7, 8, 9, 8, 9)))
LAG = 5
DEPTH = 2
STAGES = len(ENDS)
CUTS = (0,) + ENDS
OUTS = (0,) + tuple(e - LO - HI for e in ENDS[:-1]) + (NY,)
G, ZT = 4, 2
PARTS = tuple((k, lo, OUTS[k + 1]) for k, lo in enumerate(OUTS[:-2])) + tuple(
    (STAGES - 1, lo, lo + G) for lo in range(OUTS[-2], NY, G))
MESH = pl.DeviceIdType.MESH
(RIGHT, LEFT, FWD_R, FWD_L, D_OWN, D_L, D_R, D_O0, D_O1, HALO, D_HALO, HALO2) = range(12)
KINDS = 12


def kernel(frac, cost, so, co, go, value, target, obstacle, out,
           B, C, P1, Pm, Q1, Qm, A, T, O, R, ip, fp, ssem, rsem, psem, qsem, osem, lsem):
    n = lax.axis_size("gx")
    me = lax.axis_index("gx")
    j = lax.rem(me, ROW)
    base = me - j
    core = lax.rem(j, 2)
    jr, jl, jo, jp = lax.rem(j + 2, ROW), lax.rem(j + 6, ROW), lax.rem(j + 4, ROW), j + 1 - 2 * core
    qr, ql, qo = jr + 1 - 2 * core, jl + 1 - 2 * core, jo + 1 - 2 * core
    right, left, mate = base + jr, base + jl, base + jp
    up, down = lax.rem(me + ROW, n), lax.rem(me + n - ROW, n)
    beyond = jnp.where(core == 0, down + 1, up - 1)
    last = j == ROW - 1
    beside_last = j == ROW - 2

    loads = [pltpu.make_async_copy(value, B.at[j], lsem.at[0]),
             pltpu.make_async_copy(target, T, lsem.at[1]),
             pltpu.make_async_copy(obstacle, O, lsem.at[2])]
    loads[0].start()

    barrier = pltpu.get_barrier_semaphore()
    for peer in (right, left, mate, up, down, beyond):
        pl.semaphore_signal(barrier, inc=1, device_id=(peer,), device_id_type=MESH)

    loads[0].wait()
    pl.semaphore_wait(barrier, 6)

    def rank(u, _):
        mine = 2 * so[u] + co[u]
        before = 0
        for v in range(NCTRL):
            other = 2 * so[v] + co[v]
            before += jnp.where((other > mine) | ((other == mine) & (v < u)), 1, 0)
        ip[9 * NCTRL + u] = before
        return 0

    def params(k, _):
        u = 0
        for v in range(NCTRL):
            u += jnp.where(ip[9 * NCTRL + v] == k, v, 0)
        off = 2 * so[u] + co[u]
        for i in range(2):
            q = 2 * j + i + off
            d = jnp.where(q < 0, -1, jnp.where(q < RX, 0, 1))
            before = ip[(6 + i) * NCTRL]
            ip[i * NCTRL + k] = q - RX * d
            fresh = (k == 0) | (d != before)
            fp[(9 + i) * NCTRL + k] = jnp.where(fresh, jnp.inf, -jnp.inf)
            ip[(6 + i) * NCTRL] = d
            for e in (1, 2, 3):
                at = (6 + i) * NCTRL + e
                ip[at] = jnp.where(d == 2 - e, k, jnp.where(k == 0, NCTRL, ip[at]))
        ip[2 * NCTRL + k] = go[0, u]
        ip[3 * NCTRL + k] = go[1, u] + 8
        ip[4 * NCTRL + k] = (NW - go[2, u]) & (NW - 1)
        ip[5 * NCTRL + k] = (NW - 1 - go[2, u]) & (NW - 1)
        f0, f1, f2, f3 = frac[0, u], frac[1, u], frac[2, u], frac[3, u]
        fp[k] = (1.0 - f0) * (1.0 - f2)
        fp[NCTRL + k] = (1.0 - f0) * f2
        fp[2 * NCTRL + k] = f0 * (1.0 - f2)
        fp[3 * NCTRL + k] = f0 * f2
        fp[4 * NCTRL + k] = 1.0 - f1
        fp[5 * NCTRL + k] = f1
        fp[6 * NCTRL + k] = 1.0 - f3
        fp[7 * NCTRL + k] = f3
        fp[8 * NCTRL + k] = cost[u]
        return 0

    def remote(kind, k, src, dst, peer):
        return pltpu.make_async_remote_copy(src_ref=src, dst_ref=dst, send_sem=ssem.at[kind, k],
                                            recv_sem=rsem.at[kind, k], device_id=(peer,), device_id_type=MESH)

    def block(slab, k, row=None):
        ys = pl.ds(CUTS[k], CUTS[k + 1] - CUTS[k])
        return B.at[slab, :, ys] if row is None else B.at[slab, row, ys]

    def same(kind, k, peer, slab, row=None):
        return remote(kind, k, block(slab, k, row), block(slab, k, row), peer)

    def send(kind, k):
        return {
            RIGHT: lambda: same(kind, k, right, j),
            LEFT: lambda: same(kind, k, left, j),
            FWD_R: lambda: same(kind, k, right, jl, 0),
            FWD_L: lambda: same(kind, k, left, jr, 1),
            D_OWN: lambda: remote(kind, k, B.at[j], B.at[j], mate),
            D_L: lambda: same(kind, k, mate, jl),
            D_R: lambda: same(kind, k, mate, jr),
            D_O0: lambda: same(kind, k, mate, jo, 0),
            D_O1: lambda: same(kind, k, mate, jo, 1),
            HALO: lambda: remote(kind, k, block(0, k, 0), block(ROW, k, 0), down),
            D_HALO: lambda: same(kind, k, mate, ROW, 0),
            HALO2: lambda: remote(kind, k, block(0, k, 1), block(ROW, k, 1), beyond),
        }[kind]()

    def recv(kind, k):
        return {
            RIGHT: lambda: same(kind, k, right, jl),
            LEFT: lambda: same(kind, k, left, jr),
            FWD_R: lambda: same(kind, k, right, jo, 0),
            FWD_L: lambda: same(kind, k, left, jo, 1),
            D_OWN: lambda: remote(kind, k, B.at[jp], B.at[jp], mate),
            D_L: lambda: same(kind, k, mate, ql),
            D_R: lambda: same(kind, k, mate, qr),
            D_O0: lambda: same(kind, k, mate, qo, 0),
            D_O1: lambda: same(kind, k, mate, qo, 1),
            HALO: lambda: same(kind, k, down, ROW, 0),
            D_HALO: lambda: same(kind, k, mate, ROW, 0),
            HALO2: lambda: same(kind, k, beyond, ROW, 1),
        }[kind]()

    def partial(kind, part):
        ys = pl.ds(PARTS[part][1], PARTS[part][2] - PARTS[part][1])
        src, dst, peer = (Pm, Qm, up) if kind == 0 else (P1, Q1, down)
        return pltpu.make_async_remote_copy(src_ref=src.at[:, ys], dst_ref=dst.at[:, ys], send_sem=psem.at[kind, part],
                                            recv_sem=qsem.at[kind, part], device_id=(peer,), device_id_type=MESH)

    def fill(k):
        lo, hi = CUTS[k], CUTS[k + 1]

        def put(row, src, y, to):
            C[row, to, pl.ds(0, 8), :] = src[pl.ds(24, 8), :]
            C[row, to, pl.ds(8, 32), :] = src[...]
            C[row, to, pl.ds(40, 8), :] = src[pl.ds(0, 8), :]

        def one(shift, row2):
            def step(y, _):
                rows = (RX + 1,) if row2 else range(RX + 1)
                for row in rows:
                    put(row, B.at[row // 2, row % 2, y], y, y + shift)
                return 0
            return step

        lax.fori_loop(lo, hi, one(0, False), 0)
        if k == 0:
            lax.fori_loop(0, LO + HI, one(NY, False), 0)

        @pl.when(last)
        def _():
            lax.fori_loop(lo, hi, one(0, True), 0)
            if k == 0:
                lax.fori_loop(0, LO + HI, one(NY, True), 0)

    def compute(part):
        _, lo, hi = PARTS[part]

        def tile(t, _):
            i = lax.rem(t, 2)
            t = lax.div(t, 2)
            z = lax.rem(t, NZ // (8 * ZT)) * (8 * ZT)
            y = lo + lax.div(t, NZ // (8 * ZT)) * G

            def control(u, acc):
                row = ip[i * NCTRL + u]
                yy = y + LO + ip[2 * NCTRL + u]
                zz = z + ip[3 * NCTRL + u]
                s1, s2 = ip[4 * NCTRL + u], ip[5 * NCTRL + u]
                f = [fp[q * NCTRL + u] for q in range(8)]
                c, fresh = fp[8 * NCTRL + u], fp[(9 + i) * NCTRL + u]
                fields = []
                for q in range(G + 1):
                    low = f[0] * C[row, yy + q, pl.ds(zz, 8 * ZT), :] + f[1] * C[row, yy + q, pl.ds(zz + 1, 8 * ZT), :]
                    high = f[2] * C[row + 1, yy + q, pl.ds(zz, 8 * ZT), :] + f[3] * C[row + 1, yy + q, pl.ds(zz + 1, 8 * ZT), :]
                    fields.append(low + high)
                new = []
                for q in range(G):
                    h = f[4] * fields[q] + f[5] * fields[q + 1]
                    w = f[6] * pltpu.roll(h, s1, 1) + f[7] * pltpu.roll(h, s2, 1)
                    new.append(jnp.minimum(jnp.maximum(acc[q], fresh), w + c))
                    R[u, q] = new[q]
                return tuple(new)

            start = tuple([jnp.full((8 * ZT, NW), jnp.inf, jnp.float32)] * G)
            lax.fori_loop(0, NCTRL, control, start, unroll=True)
            zs = pl.ds(pl.multiple_of(z, 8), 8 * ZT)
            for q in range(G):
                for e, ref in ((1, P1), (2, A), (3, Pm)):
                    ref[i, y + q, zs, :] = R[ip[(6 + i) * NCTRL + e], q]
            return 0

        lax.fori_loop(0, 2 * ((hi - lo) // G) * (NZ // (8 * ZT)), tile, 0)

    def combine(part):
        partial(0, part).wait_recv()
        partial(1, part).wait_recv()
        _, lo, hi = PARTS[part]

        def step(y, _):
            at = lax.rem(y + LO, NY)
            for i in range(2):
                best = jnp.minimum(A[i, y], jnp.minimum(Q1[i, y], Qm[i, y]))
                A[i, y] = jnp.maximum(O[i, at], jnp.minimum(T[i, at], best))
            return 0

        lax.fori_loop(lo, hi, step, 0)

    def own(k):
        if k < STAGES:
            send(RIGHT, k).start()
            send(LEFT, k).start()

    def halo(k, which):
        @pl.when(which)
        def _():
            send(HALO, k).start()

    def neighbours(k):
        recv(RIGHT, k).wait_recv()
        send(FWD_R, k).start()
        send(D_L, k).start()
        halo(k, j == 2)
        recv(LEFT, k).wait_recv()
        send(FWD_L, k).start()
        send(D_R, k).start()
        halo(k, j == 6)

        @pl.when(beside_last)
        def _():
            send(HALO2, k).start()

        own(k + DEPTH)

    def opposite(k):
        recv(FWD_R, k).wait_recv()
        send(D_O0, k).start()
        halo(k, j == 4)
        recv(FWD_L, k).wait_recv()
        send(D_O1, k).start()

    def pass_halo(k):
        @pl.when(core == 0)
        def _():
            recv(HALO, k).wait_recv()
            send(D_HALO, k).start()

    def work(k):
        if k == 0:
            recv(D_OWN, 0).wait_recv()
        for kind in (D_L, D_R, D_O0, D_O1):
            recv(kind, k).wait_recv()

        @pl.when(core == 1)
        def _():
            recv(D_HALO, k).wait_recv()

        @pl.when(last)
        def _():
            recv(HALO2, k).wait_recv()

        fill(k)
        for part, (stage, _, _) in enumerate(PARTS):
            if stage == k:
                compute(part)
                partial(0, part).start()
                partial(1, part).start()

    def store(part):
        _, lo, hi = PARTS[part]
        return pltpu.make_async_copy(A.at[:, pl.ds(lo, hi - lo)], out.at[:, pl.ds((lo + LO) % NY, hi - lo)],
                                     osem.at[part])

    def finish(stage):
        for part, (k, _, _) in enumerate(PARTS):
            if k == stage:
                combine(part)
                store(part).start()

    def drain():
        send(D_OWN, 0).wait_send()
        for k in range(STAGES):
            for kind in (RIGHT, LEFT, FWD_R, FWD_L, D_L, D_R, D_O0, D_O1):
                send(kind, k).wait_send()

            @pl.when(core == 0)
            def _():
                send(HALO, k).wait_send()
                send(D_HALO, k).wait_send()

            @pl.when(beside_last)
            def _():
                send(HALO2, k).wait_send()

    for k in range(DEPTH):
        own(k)
    send(D_OWN, 0).start()
    for k in range(STAGES):
        halo(k, j == 0)
    loads[1].start()
    loads[2].start()
    R[NCTRL] = jnp.full(R.shape[1:], jnp.inf, jnp.float32)
    for i in range(2):
        ip[(6 + i) * NCTRL] = 0
        for e in (1, 2, 3):
            ip[(6 + i) * NCTRL + e] = 0
    lax.fori_loop(0, NCTRL, rank, 0)
    lax.fori_loop(0, NCTRL, params, 0)
    for what, k in ORDER:
        if what == "N":
            neighbours(k)
        elif what == "O":
            opposite(k)
        elif what == "H":
            pass_halo(k)
        else:
            work(k)
            if k == 1:
                loads[1].wait()
                loads[2].wait()
            if k >= LAG:
                finish(k - LAG)
    drain()
    for k in range(STAGES - LAG, STAGES):
        finish(k)

    for part in range(len(PARTS)):
        partial(0, part).wait_send()
        partial(1, part).wait_send()
    for part in range(len(PARTS)):
        store(part).wait()


def body(value, target, obstacle, fractions, control_cost, shard_offset, cell_offset, grid_offset):
    slab = (CX, NY, NZ, NW)
    vmem = functools.partial(pltpu.VMEM, dtype=jnp.float32)
    smem = pl.BlockSpec(memory_space=pltpu.SMEM)
    anywhere = pl.BlockSpec(memory_space=pl.ANY)
    return pl.pallas_call(
        kernel,
        name="reach_avoid",
        out_shape=jax.ShapeDtypeStruct(slab, jnp.float32),
        in_specs=[smem] * 5 + [anywhere] * 3,
        out_specs=anywhere,
        scratch_shapes=[
            vmem((ROW + 1,) + slab),
            vmem((RX + 2, NY + LO + HI, NZ + 16, NW)),
            vmem(slab), vmem(slab), vmem(slab), vmem(slab), vmem(slab), vmem(slab), vmem(slab),
            vmem((NCTRL + 1, G, 8 * ZT, NW)),
            pltpu.SMEM((10 * NCTRL,), jnp.int32),
            pltpu.SMEM((11 * NCTRL,), jnp.float32),
            pltpu.SemaphoreType.DMA((KINDS, STAGES)),
            pltpu.SemaphoreType.DMA((KINDS, STAGES)),
            pltpu.SemaphoreType.DMA((2, len(PARTS))),
            pltpu.SemaphoreType.DMA((2, len(PARTS))),
            pltpu.SemaphoreType.DMA((len(PARTS),)),
            pltpu.SemaphoreType.DMA((3,)),
        ],
        compiler_params=pltpu.CompilerParams(collective_id=0, has_side_effects=True, vmem_limit_bytes=62 << 20),
    )(fractions.T, control_cost, shard_offset, cell_offset, grid_offset.T, value, target, obstacle)


def solution(mesh):
    grid = P("gx", None, None, None)
    return jax.shard_map(body, mesh=mesh, in_specs=(grid, grid, grid, P(), P(), P(), P(), P()), out_specs=grid,
                         check_vma=False)
```

```python
import functools

import jax
import jax.numpy as jnp
from jax import lax
from jax.experimental import pallas as pl
from jax.experimental.pallas import tpu as pltpu
from jax.sharding import PartitionSpec as P

CX, NY, NZ, NW, NCTRL = 2, 48, 32, 128, 16
ROW = 8
RX = ROW * CX
LO, HI = 4, 5
ENDS = (13, 17, 21, 25, 29, 33, 37, 41, 45, 48)
ORDER = tuple(zip("NNONOHWNOHWNOHWNOHWNOHWNOHWNWOHNWOHWOHW", (0, 1, 0, 2, 1, 0, 0, 3, 2, 1, 1, 4, 3, 2, 2, 5, 4, 3, 3, 6, 5, 4, 4, 7, 6, 5, 5, 8, 6, 7, 6, 9, 7, 8, 7, 8, 9, 8, 9)))
LAG = 5
DEPTH = 2
STAGES = len(ENDS)
CUTS = (0,) + ENDS
OUTS = (0,) + tuple(e - LO - HI for e in ENDS[:-1]) + (NY,)
G, ZT = 4, 2
PARTS = tuple((k, lo, OUTS[k + 1]) for k, lo in enumerate(OUTS[:-2])) + tuple(
    (STAGES - 1, lo, lo + G) for lo in range(OUTS[-2], NY, G))
MESH = pl.DeviceIdType.MESH
SPANS = tuple((ENDS[min(k, STAGES - 1)] if k else 0, ENDS[min(k + 1, STAGES - 1)]) for k in range(STAGES))
SPANS = (SPANS, tuple(zip(CUTS[:-1], CUTS[1:])))
MOVED = tuple(SPANS[0][k][1] - SPANS[0][k][0] + CUTS[k + 1] - CUTS[k] for k in range(STAGES))
(RIGHT, LEFT, FWD_R, FWD_L, D_OWN, D_L, D_R, D_O, HALO, D_HALO, HALO2, D_HALO2, PART, STORE) = range(14)
(A_RIGHT, A_LEFT, A_FWD, A_D, A_HALO, A_D_HALO, A_HALO2, A_D_HALO2) = range(8)

def kernel(frac, cost, so, co, go, value, target, obstacle, out,
           B, C, P1, Pm, Q1, Qm, A, T, O, R, ip, fp, ssem, rsem, qsem, lsem, ysem):
    n = lax.axis_size("gx")
    me = lax.axis_index("gx")
    j = lax.rem(me, ROW)
    base = me - j
    core = lax.rem(j, 2)
    jr, jl, jo, jp = lax.rem(j + 2, ROW), lax.rem(j + 6, ROW), lax.rem(j + 4, ROW), j + 1 - 2 * core
    qr, ql, qo = jr + 1 - 2 * core, jl + 1 - 2 * core, jo + 1 - 2 * core
    right, left, mate = base + jr, base + jl, base + jp
    up, down = lax.rem(me + ROW, n), lax.rem(me + n - ROW, n)
    last = j == ROW - 1
    beside_last = j == ROW - 2

    loads = [pltpu.make_async_copy(value, B.at[j], lsem.at[0]),
             pltpu.make_async_copy(target, T, lsem.at[1]),
             pltpu.make_async_copy(obstacle, O, lsem.at[2])]
    loads[0].start()

    barrier = pltpu.get_barrier_semaphore()
    for peer in (right, left, mate, down):
        pl.semaphore_signal(barrier, inc=1, device_id=(peer,), device_id_type=MESH)

    loads[0].wait()
    pl.semaphore_wait(barrier, 4)
    pl.semaphore_signal(ysem, inc=1, device_id=(up,), device_id_type=MESH)

    def rank(u, _):
        mine = 2 * so[u] + co[u]
        before = 0
        for v in range(NCTRL):
            other = 2 * so[v] + co[v]
            before += jnp.where((other > mine) | ((other == mine) & (v < u)), 1, 0)
        ip[9 * NCTRL + u] = before
        return 0

    def params(k, _):
        u = 0
        for v in range(NCTRL):
            u += jnp.where(ip[9 * NCTRL + v] == k, v, 0)
        off = 2 * so[u] + co[u]
        for i in range(2):
            q = 2 * j + i + off
            d = jnp.where(q < 0, -1, jnp.where(q < RX, 0, 1))
            before = ip[(6 + i) * NCTRL]
            ip[i * NCTRL + k] = q - RX * d
            fresh = (k == 0) | (d != before)
            fp[(9 + i) * NCTRL + k] = jnp.where(fresh, jnp.inf, -jnp.inf)
            ip[(6 + i) * NCTRL] = d
            for e in (1, 2, 3):
                at = (6 + i) * NCTRL + e
                ip[at] = jnp.where(d == 2 - e, k, jnp.where(k == 0, NCTRL, ip[at]))
        ip[2 * NCTRL + k] = go[0, u]
        ip[3 * NCTRL + k] = go[1, u] + 8
        ip[4 * NCTRL + k] = (NW - go[2, u]) & (NW - 1)
        ip[5 * NCTRL + k] = (NW - 1 - go[2, u]) & (NW - 1)
        f0, f1, f2, f3 = frac[0, u], frac[1, u], frac[2, u], frac[3, u]
        fp[k] = (1.0 - f0) * (1.0 - f2)
        fp[NCTRL + k] = (1.0 - f0) * f2
        fp[2 * NCTRL + k] = f0 * (1.0 - f2)
        fp[3 * NCTRL + k] = f0 * f2
        fp[4 * NCTRL + k] = 1.0 - f1
        fp[5 * NCTRL + k] = f1
        fp[6 * NCTRL + k] = 1.0 - f3
        fp[7 * NCTRL + k] = f3
        fp[8 * NCTRL + k] = cost[u]
        return 0

    def remote(out_sem, in_sem, src, dst, peer):
        return pltpu.make_async_remote_copy(src_ref=src, dst_ref=dst, send_sem=out_sem, recv_sem=in_sem,
                                            device_id=(peer,), device_id_type=MESH)

    def move(kind, arrival, k, peer, slab, rows, to=None):
        for row in rows:
            lo, hi = SPANS[row][k]
            if lo < hi:
                ys = pl.ds(lo, hi - lo)
                remote(ssem.at[kind], rsem.at[arrival, k], B.at[slab, row, ys],
                       B.at[slab if to is None else to, row, ys], peer).start()

    def arrived(arrival, k, peer, cells, slabs=1):
        some = B.at[pl.ds(0, slabs), 0, pl.ds(0, cells)]
        remote(ssem.at[RIGHT], rsem.at[arrival, k], some, some, peer).wait_recv()

    def sent(kind, ref):
        remote(ssem.at[kind], rsem.at[A_RIGHT, 0], ref, ref, right).wait_send()

    def partials(part):
        _, lo, hi = PARTS[part]
        ys = pl.ds(lo, hi - lo)
        for src, dst, peer in ((Pm, Qm, up), (P1, Q1, down)):
            remote(ssem.at[PART], qsem.at[part], src.at[:, ys], dst.at[:, ys], peer).start()

    def fill(k):
        lo, hi = CUTS[k], CUTS[k + 1]

        def put(row, src, y, to):
            C[row, to, pl.ds(0, 8), :] = src[pl.ds(24, 8), :]
            C[row, to, pl.ds(8, 32), :] = src[...]
            C[row, to, pl.ds(40, 8), :] = src[pl.ds(0, 8), :]

        def one(shift, row2):
            def step(y, _):
                rows = (RX + 1,) if row2 else range(RX + 1)
                for row in rows:
                    put(row, B.at[row // 2, row % 2, y], y, y + shift)
                return 0
            return step

        lax.fori_loop(lo, hi, one(0, False), 0)
        if k == 0:
            lax.fori_loop(0, LO + HI, one(NY, False), 0)

        @pl.when(last)
        def _():
            lax.fori_loop(lo, hi, one(0, True), 0)
            if k == 0:
                lax.fori_loop(0, LO + HI, one(NY, True), 0)

    def compute(part):
        _, lo, hi = PARTS[part]

        def tile(t, _):
            i = lax.rem(t, 2)
            t = lax.div(t, 2)
            z = lax.rem(t, NZ // (8 * ZT)) * (8 * ZT)
            y = lo + lax.div(t, NZ // (8 * ZT)) * G

            def control(u, acc):
                row = ip[i * NCTRL + u]
                yy = y + LO + ip[2 * NCTRL + u]
                zz = z + ip[3 * NCTRL + u]
                s1, s2 = ip[4 * NCTRL + u], ip[5 * NCTRL + u]
                f = [fp[q * NCTRL + u] for q in range(8)]
                c, fresh = fp[8 * NCTRL + u], fp[(9 + i) * NCTRL + u]
                fields = []
                for q in range(G + 1):
                    low = f[0] * C[row, yy + q, pl.ds(zz, 8 * ZT), :] + f[1] * C[row, yy + q, pl.ds(zz + 1, 8 * ZT), :]
                    high = f[2] * C[row + 1, yy + q, pl.ds(zz, 8 * ZT), :] + f[3] * C[row + 1, yy + q, pl.ds(zz + 1, 8 * ZT), :]
                    fields.append(low + high)
                new = []
                for q in range(G):
                    h = f[4] * fields[q] + f[5] * fields[q + 1]
                    w = f[6] * pltpu.roll(h, s1, 1) + f[7] * pltpu.roll(h, s2, 1)
                    new.append(jnp.minimum(jnp.maximum(acc[q], fresh), w + c))
                    R[u, q] = new[q]
                return tuple(new)

            start = tuple([jnp.full((8 * ZT, NW), jnp.inf, jnp.float32)] * G)
            lax.fori_loop(0, NCTRL, control, start, unroll=True)
            zs = pl.ds(pl.multiple_of(z, 8), 8 * ZT)
            for q in range(G):
                for e, ref in ((1, P1), (2, A), (3, Pm)):
                    ref[i, y + q, zs, :] = R[ip[(6 + i) * NCTRL + e], q]
            return 0

        lax.fori_loop(0, 2 * ((hi - lo) // G) * (NZ // (8 * ZT)), tile, 0)

    def combine(part):
        _, lo, hi = PARTS[part]
        some = Q1.at[:, pl.ds(0, 2 * (hi - lo))]
        remote(ssem.at[PART], qsem.at[part], some, some, down).wait_recv()

        def step(y, _):
            at = lax.rem(y + LO, NY)
            for i in range(2):
                best = jnp.minimum(A[i, y], jnp.minimum(Q1[i, y], Qm[i, y]))
                A[i, y] = jnp.maximum(O[i, at], jnp.minimum(T[i, at], best))
            return 0

        lax.fori_loop(lo, hi, step, 0)

    def own(k):
        if k < STAGES:
            move(RIGHT, A_RIGHT, k, right, j, (0, 1))
            move(LEFT, A_LEFT, k, left, j, (0, 1))

    def halo(k, which):
        @pl.when(which)
        def _():
            move(HALO, A_HALO, k, down, 0, (0,), ROW)

    def neighbours(k):
        arrived(A_RIGHT, k, right, MOVED[k])
        move(FWD_R, A_FWD, k, right, jl, (0,))
        move(D_L, A_D, k, mate, jl, (0, 1))
        if k == 0:
            pl.semaphore_wait(ysem, 1)
            for early in range(STAGES):
                halo(early, j == 0)
        halo(k, j == 2)
        arrived(A_LEFT, k, left, MOVED[k])
        move(FWD_L, A_FWD, k, left, jr, (1,))
        move(D_R, A_D, k, mate, jr, (0, 1))
        halo(k, beside_last)

        @pl.when(beside_last)
        def _():
            move(HALO2, A_HALO2, k, down, 0, (1,), ROW)

        own(k + DEPTH)

    def opposite(k):
        arrived(A_FWD, k, right, MOVED[k])
        halo(k, j == 4)
        move(D_O, A_D, k, mate, jo, (0, 1))

    def pass_halo(k):
        @pl.when(core == 0)
        def _():
            arrived(A_HALO, k, down, SPANS[0][k][1] - SPANS[0][k][0])
            move(D_HALO, A_D_HALO, k, mate, ROW, (0,))

    def work(k):
        @pl.when(beside_last)
        def _():
            arrived(A_HALO2, k, down, CUTS[k + 1] - CUTS[k])
            move(D_HALO2, A_D_HALO2, k, mate, ROW, (1,))

        if k == 0:
            remote(ssem.at[D_OWN], rsem.at[A_D, STAGES], B.at[jp], B.at[jp], mate).wait_recv()
        arrived(A_D, k, mate, MOVED[k], 3)
        if k != 1:
            ahead = max(k - 1, 0)

            @pl.when(core == 1)
            def _():
                arrived(A_D_HALO, ahead, mate, SPANS[0][ahead][1] - SPANS[0][ahead][0])

        @pl.when(last)
        def _():
            arrived(A_D_HALO2, k, mate, CUTS[k + 1] - CUTS[k])

        fill(k)
        for part, (stage, _, _) in enumerate(PARTS):
            if stage == k:
                compute(part)
                partials(part)

    def store(part):
        _, lo, hi = PARTS[part]
        return pltpu.make_async_copy(A.at[:, pl.ds(lo, hi - lo)], out.at[:, pl.ds((lo + LO) % NY, hi - lo)],
                                     ssem.at[STORE])

    def finish(stage):
        for part, (k, _, _) in enumerate(PARTS):
            if k == stage:
                combine(part)
                store(part).start()

    def drain():
        for kind, ref in ((RIGHT, B.at[j]), (LEFT, B.at[j]), (FWD_R, B.at[jl, 0]), (FWD_L, B.at[jr, 1]), (D_OWN, B.at[j]),
                          (D_L, B.at[jl]), (D_R, B.at[jr]), (D_O, B.at[jo])):
            sent(kind, ref)

        @pl.when(core == 0)
        def _():
            sent(HALO, B.at[0, 0])
            sent(D_HALO, B.at[ROW, 0])

        @pl.when(beside_last)
        def _():
            sent(HALO2, B.at[0, 1])
            sent(D_HALO2, B.at[ROW, 1])

    for k in range(DEPTH):
        own(k)
    remote(ssem.at[D_OWN], rsem.at[A_D, STAGES], B.at[j], B.at[j], mate).start()
    loads[1].start()
    loads[2].start()
    R[NCTRL] = jnp.full(R.shape[1:], jnp.inf, jnp.float32)
    for i in range(2):
        ip[(6 + i) * NCTRL] = 0
        for e in (1, 2, 3):
            ip[(6 + i) * NCTRL + e] = 0
    lax.fori_loop(0, NCTRL, rank, 0)
    lax.fori_loop(0, NCTRL, params, 0)
    for what, k in ORDER:
        if what == "N":
            neighbours(k)
        elif what == "O":
            opposite(k)
        elif what == "H":
            pass_halo(k)
        else:
            work(k)
            if k == 1:
                loads[1].wait()
                loads[2].wait()
            if k >= LAG:
                finish(k - LAG)
    drain()
    for k in range(STAGES - LAG, STAGES):
        finish(k)

    sent(PART, B.at[pl.ds(0, 2)])
    pltpu.make_async_copy(A, out, ssem.at[STORE]).wait()


def body(value, target, obstacle, fractions, control_cost, shard_offset, cell_offset, grid_offset):
    slab = (CX, NY, NZ, NW)
    vmem = functools.partial(pltpu.VMEM, dtype=jnp.float32)
    smem = pl.BlockSpec(memory_space=pltpu.SMEM)
    anywhere = pl.BlockSpec(memory_space=pl.ANY)
    return pl.pallas_call(
        kernel,
        name="reach_avoid",
        out_shape=jax.ShapeDtypeStruct(slab, jnp.float32),
        in_specs=[smem] * 5 + [anywhere] * 3,
        out_specs=anywhere,
        scratch_shapes=[
            vmem((ROW + 1,) + slab),
            vmem((RX + 2, NY + LO + HI, NZ + 16, NW)),
            vmem(slab), vmem(slab), vmem(slab), vmem(slab), vmem(slab), vmem(slab), vmem(slab),
            vmem((NCTRL + 1, G, 8 * ZT, NW)),
            pltpu.SMEM((10 * NCTRL,), jnp.int32),
            pltpu.SMEM((11 * NCTRL,), jnp.float32),
            pltpu.SemaphoreType.DMA((14,)),
            pltpu.SemaphoreType.DMA((8, STAGES + 1)),
            pltpu.SemaphoreType.DMA((len(PARTS),)),
            pltpu.SemaphoreType.DMA((3,)),
            pltpu.SemaphoreType.REGULAR,
        ],
        compiler_params=pltpu.CompilerParams(collective_id=0, has_side_effects=True, vmem_limit_bytes=62 << 20),
    )(fractions.T, control_cost, shard_offset, cell_offset, grid_offset.T, value, target, obstacle)


def solution(mesh):
    grid = P("gx", None, None, None)
    return jax.shard_map(body, mesh=mesh, in_specs=(grid, grid, grid, P(), P(), P(), P(), P()), out_specs=grid,
                         check_vma=False)
```

```python
import functools

import jax
import jax.numpy as jnp
from jax import lax
from jax.experimental import pallas as pl
from jax.experimental.pallas import tpu as pltpu
from jax.sharding import PartitionSpec as P

CX, NY, NZ, NW, NCTRL = 2, 48, 32, 128, 16
ROW = 8
RX = ROW * CX
LO, HI = 4, 5
ENDS = (9, 13, 17, 21, 25, 29, 33, 37, 41, 45, 48)
ORDER = tuple(zip("NNONOHWNOHWNOHWNOHWNOHWNOHWNOHWNWOHNWOHWOHW", (0, 1, 0, 2, 1, 0, 0, 3, 2, 1, 1, 4, 3, 2, 2, 5, 4, 3, 3, 6, 5, 4, 4, 7, 6, 5, 5, 8, 7, 6, 6, 9, 7, 8, 7, 10, 8, 9, 8, 9, 10, 9, 10)))
LAG = 5
LEAD = 1
DEPTH = 2
STAGES = len(ENDS)
CUTS = (0,) + ENDS
OUTS = (0,) + tuple(max(e - LO - HI, 0) for e in ENDS[:-1]) + (NY,)
G, ZT = 4, 2
PARTS = tuple((k, lo, OUTS[k + 1]) for k, lo in enumerate(OUTS[:-2]) if lo < OUTS[k + 1]) + tuple(
    (STAGES - 1, lo, lo + G) for lo in range(OUTS[-2], NY, G))
MESH = pl.DeviceIdType.MESH
SPANS = tuple((ENDS[min(k + LEAD - 1, STAGES - 1)] if k else 0, ENDS[min(k + LEAD, STAGES - 1)]) for k in range(STAGES))
SPANS = (SPANS, tuple(zip(CUTS[:-1], CUTS[1:])))
MOVED = tuple(SPANS[0][k][1] - SPANS[0][k][0] + CUTS[k + 1] - CUTS[k] for k in range(STAGES))
(RIGHT, LEFT, FWD_R, FWD_L, D_OWN, D_L, D_R, D_O, HALO, D_HALO, HALO2, D_HALO2, PART, STORE) = range(14)
(A_RIGHT, A_LEFT, A_FWD, A_D, A_HALO, A_D_HALO, A_HALO2, A_D_HALO2) = range(8)

def kernel(frac, cost, so, co, go, value, target, obstacle, out,
           B, C, P1, Pm, Q1, Qm, A, T, O, R, ip, fp, ssem, rsem, qsem, lsem, ysem):
    n = lax.axis_size("gx")
    me = lax.axis_index("gx")
    j = lax.rem(me, ROW)
    base = me - j
    core = lax.rem(j, 2)
    jr, jl, jo, jp = lax.rem(j + 2, ROW), lax.rem(j + 6, ROW), lax.rem(j + 4, ROW), j + 1 - 2 * core
    qr, ql, qo = jr + 1 - 2 * core, jl + 1 - 2 * core, jo + 1 - 2 * core
    right, left, mate = base + jr, base + jl, base + jp
    up, down = lax.rem(me + ROW, n), lax.rem(me + n - ROW, n)
    last = j == ROW - 1
    beside_last = j == ROW - 2

    loads = [pltpu.make_async_copy(value, B.at[j], lsem.at[0]),
             pltpu.make_async_copy(target, T, lsem.at[1]),
             pltpu.make_async_copy(obstacle, O, lsem.at[2])]
    loads[0].start()

    barrier = pltpu.get_barrier_semaphore()
    for peer in (right, left, mate, down):
        pl.semaphore_signal(barrier, inc=1, device_id=(peer,), device_id_type=MESH)

    loads[0].wait()
    pl.semaphore_wait(barrier, 4)
    pl.semaphore_signal(ysem, inc=1, device_id=(up,), device_id_type=MESH)

    def rank(u, _):
        mine = 2 * so[u] + co[u]
        before = 0
        for v in range(NCTRL):
            other = 2 * so[v] + co[v]
            before += jnp.where((other > mine) | ((other == mine) & (v < u)), 1, 0)
        ip[9 * NCTRL + u] = before
        return 0

    def params(k, _):
        u = 0
        for v in range(NCTRL):
            u += jnp.where(ip[9 * NCTRL + v] == k, v, 0)
        off = 2 * so[u] + co[u]
        for i in range(2):
            q = 2 * j + i + off
            d = jnp.where(q < 0, -1, jnp.where(q < RX, 0, 1))
            before = ip[(6 + i) * NCTRL]
            ip[i * NCTRL + k] = q - RX * d
            fresh = (k == 0) | (d != before)
            fp[(9 + i) * NCTRL + k] = jnp.where(fresh, jnp.inf, -jnp.inf)
            ip[(6 + i) * NCTRL] = d
            for e in (1, 2, 3):
                at = (6 + i) * NCTRL + e
                ip[at] = jnp.where(d == 2 - e, k, jnp.where(k == 0, NCTRL, ip[at]))
        ip[2 * NCTRL + k] = go[0, u]
        ip[3 * NCTRL + k] = go[1, u] + 8
        ip[4 * NCTRL + k] = (NW - go[2, u]) & (NW - 1)
        ip[5 * NCTRL + k] = (NW - 1 - go[2, u]) & (NW - 1)
        f0, f1, f2, f3 = frac[0, u], frac[1, u], frac[2, u], frac[3, u]
        fp[k] = (1.0 - f0) * (1.0 - f2)
        fp[NCTRL + k] = (1.0 - f0) * f2
        fp[2 * NCTRL + k] = f0 * (1.0 - f2)
        fp[3 * NCTRL + k] = f0 * f2
        fp[4 * NCTRL + k] = 1.0 - f1
        fp[5 * NCTRL + k] = f1
        fp[6 * NCTRL + k] = 1.0 - f3
        fp[7 * NCTRL + k] = f3
        fp[8 * NCTRL + k] = cost[u]
        return 0

    def remote(out_sem, in_sem, src, dst, peer):
        return pltpu.make_async_remote_copy(src_ref=src, dst_ref=dst, send_sem=out_sem, recv_sem=in_sem,
                                            device_id=(peer,), device_id_type=MESH)

    def move(kind, arrival, k, peer, slab, rows, to=None):
        for row in rows:
            lo, hi = SPANS[row][k]
            if lo < hi:
                ys = pl.ds(lo, hi - lo)
                remote(ssem.at[kind], rsem.at[arrival, k], B.at[slab, row, ys],
                       B.at[slab if to is None else to, row, ys], peer).start()

    def arrived(arrival, k, peer, cells, slabs=1):
        some = B.at[pl.ds(0, slabs), 0, pl.ds(0, cells)]
        remote(ssem.at[RIGHT], rsem.at[arrival, k], some, some, peer).wait_recv()

    def sent(kind, ref):
        remote(ssem.at[kind], rsem.at[A_RIGHT, 0], ref, ref, right).wait_send()

    def partials(part):
        _, lo, hi = PARTS[part]
        ys = pl.ds(lo, hi - lo)
        for src, dst, peer in ((Pm, Qm, up), (P1, Q1, down)):
            remote(ssem.at[PART], qsem.at[part], src.at[:, ys], dst.at[:, ys], peer).start()

    def fill(k):
        lo, hi = CUTS[k], CUTS[k + 1]

        def put(row, src, y, to):
            C[row, to, pl.ds(0, 8), :] = src[pl.ds(24, 8), :]
            C[row, to, pl.ds(8, 32), :] = src[...]
            C[row, to, pl.ds(40, 8), :] = src[pl.ds(0, 8), :]

        def one(shift, row2):
            def step(y, _):
                rows = (RX + 1,) if row2 else range(RX + 1)
                for row in rows:
                    put(row, B.at[row // 2, row % 2, y], y, y + shift)
                return 0
            return step

        lax.fori_loop(lo, hi, one(0, False), 0)
        if k == 0:
            lax.fori_loop(0, LO + HI, one(NY, False), 0)

        @pl.when(last)
        def _():
            lax.fori_loop(lo, hi, one(0, True), 0)
            if k == 0:
                lax.fori_loop(0, LO + HI, one(NY, True), 0)

    def compute(part):
        _, lo, hi = PARTS[part]

        def tile(t, _):
            i = lax.rem(t, 2)
            t = lax.div(t, 2)
            z = lax.rem(t, NZ // (8 * ZT)) * (8 * ZT)
            y = lo + lax.div(t, NZ // (8 * ZT)) * G

            def control(u, acc):
                row = ip[i * NCTRL + u]
                yy = y + LO + ip[2 * NCTRL + u]
                zz = z + ip[3 * NCTRL + u]
                s1, s2 = ip[4 * NCTRL + u], ip[5 * NCTRL + u]
                f = [fp[q * NCTRL + u] for q in range(8)]
                c, fresh = fp[8 * NCTRL + u], fp[(9 + i) * NCTRL + u]
                fields = []
                for q in range(G + 1):
                    low = f[0] * C[row, yy + q, pl.ds(zz, 8 * ZT), :] + f[1] * C[row, yy + q, pl.ds(zz + 1, 8 * ZT), :]
                    high = f[2] * C[row + 1, yy + q, pl.ds(zz, 8 * ZT), :] + f[3] * C[row + 1, yy + q, pl.ds(zz + 1, 8 * ZT), :]
                    fields.append(low + high)
                new = []
                for q in range(G):
                    h = f[4] * fields[q] + f[5] * fields[q + 1]
                    w = f[6] * pltpu.roll(h, s1, 1) + f[7] * pltpu.roll(h, s2, 1)
                    new.append(jnp.minimum(jnp.maximum(acc[q], fresh), w + c))
                    R[u, q] = new[q]
                return tuple(new)

            start = tuple([jnp.full((8 * ZT, NW), jnp.inf, jnp.float32)] * G)
            lax.fori_loop(0, NCTRL, control, start, unroll=True)
            zs = pl.ds(pl.multiple_of(z, 8), 8 * ZT)
            for q in range(G):
                for e, ref in ((1, P1), (2, A), (3, Pm)):
                    ref[i, y + q, zs, :] = R[ip[(6 + i) * NCTRL + e], q]
            return 0

        lax.fori_loop(0, 2 * ((hi - lo) // G) * (NZ // (8 * ZT)), tile, 0)

    def combine(part):
        _, lo, hi = PARTS[part]
        some = Q1.at[:, pl.ds(0, 2 * (hi - lo))]
        remote(ssem.at[PART], qsem.at[part], some, some, down).wait_recv()

        def step(y, _):
            at = lax.rem(y + LO, NY)
            for i in range(2):
                best = jnp.minimum(A[i, y], jnp.minimum(Q1[i, y], Qm[i, y]))
                A[i, y] = jnp.maximum(O[i, at], jnp.minimum(T[i, at], best))
            return 0

        lax.fori_loop(lo, hi, step, 0)

    def own(k):
        if k < STAGES:
            move(RIGHT, A_RIGHT, k, right, j, (0, 1))
            move(LEFT, A_LEFT, k, left, j, (0, 1))

    def halo(k, which):
        @pl.when(which)
        def _():
            move(HALO, A_HALO, k, down, 0, (0,), ROW)

    def neighbours(k):
        arrived(A_RIGHT, k, right, MOVED[k])
        move(FWD_R, A_FWD, k, right, jl, (0,))
        move(D_L, A_D, k, mate, jl, (0, 1))
        if k == 0:
            pl.semaphore_wait(ysem, 1)
            for early in range(STAGES):
                halo(early, j == 0)
        halo(k, j == 2)
        arrived(A_LEFT, k, left, MOVED[k])
        move(FWD_L, A_FWD, k, left, jr, (1,))
        move(D_R, A_D, k, mate, jr, (0, 1))
        halo(k, beside_last)

        @pl.when(beside_last)
        def _():
            move(HALO2, A_HALO2, k, down, 0, (1,), ROW)

        own(k + DEPTH)

    def opposite(k):
        arrived(A_FWD, k, right, MOVED[k])
        halo(k, j == 4)
        move(D_O, A_D, k, mate, jo, (0, 1))

    def pass_halo(k):
        @pl.when(core == 0)
        def _():
            arrived(A_HALO, k, down, SPANS[0][k][1] - SPANS[0][k][0])
            move(D_HALO, A_D_HALO, k, mate, ROW, (0,))

    def work(k):
        @pl.when(beside_last)
        def _():
            arrived(A_HALO2, k, down, CUTS[k + 1] - CUTS[k])
            move(D_HALO2, A_D_HALO2, k, mate, ROW, (1,))

        if k == 0:
            remote(ssem.at[D_OWN], rsem.at[A_D, STAGES], B.at[jp], B.at[jp], mate).wait_recv()
        arrived(A_D, k, mate, MOVED[k], 3)
        if k == 0 or k > LEAD:
            ahead = max(k - LEAD, 0)

            @pl.when(core == 1)
            def _():
                arrived(A_D_HALO, ahead, mate, SPANS[0][ahead][1] - SPANS[0][ahead][0])

        @pl.when(last)
        def _():
            arrived(A_D_HALO2, k, mate, CUTS[k + 1] - CUTS[k])

        fill(k)
        for part, (stage, _, _) in enumerate(PARTS):
            if stage == k:
                compute(part)
                partials(part)

    def store(part):
        _, lo, hi = PARTS[part]
        return pltpu.make_async_copy(A.at[:, pl.ds(lo, hi - lo)], out.at[:, pl.ds((lo + LO) % NY, hi - lo)],
                                     ssem.at[STORE])

    def finish(stage):
        for part, (k, _, _) in enumerate(PARTS):
            if k == stage:
                combine(part)
                store(part).start()

    def drain():
        for kind, ref in ((RIGHT, B.at[j]), (LEFT, B.at[j]), (FWD_R, B.at[jl, 0]), (FWD_L, B.at[jr, 1]), (D_OWN, B.at[j]),
                          (D_L, B.at[jl]), (D_R, B.at[jr]), (D_O, B.at[jo])):
            sent(kind, ref)

        @pl.when(core == 0)
        def _():
            sent(HALO, B.at[0, 0])
            sent(D_HALO, B.at[ROW, 0])

        @pl.when(beside_last)
        def _():
            sent(HALO2, B.at[0, 1])
            sent(D_HALO2, B.at[ROW, 1])

    for k in range(DEPTH):
        own(k)
    remote(ssem.at[D_OWN], rsem.at[A_D, STAGES], B.at[j], B.at[j], mate).start()
    loads[1].start()
    loads[2].start()
    R[NCTRL] = jnp.full(R.shape[1:], jnp.inf, jnp.float32)
    for i in range(2):
        ip[(6 + i) * NCTRL] = 0
        for e in (1, 2, 3):
            ip[(6 + i) * NCTRL + e] = 0
    lax.fori_loop(0, NCTRL, rank, 0)
    lax.fori_loop(0, NCTRL, params, 0)
    for what, k in ORDER:
        if what == "N":
            neighbours(k)
        elif what == "O":
            opposite(k)
        elif what == "H":
            pass_halo(k)
        else:
            work(k)
            if k == 1:
                loads[1].wait()
                loads[2].wait()
            if k >= LAG:
                finish(k - LAG)
    drain()
    for k in range(STAGES - LAG, STAGES):
        finish(k)

    sent(PART, B.at[pl.ds(0, 2)])
    pltpu.make_async_copy(A, out, ssem.at[STORE]).wait()


def body(value, target, obstacle, fractions, control_cost, shard_offset, cell_offset, grid_offset):
    slab = (CX, NY, NZ, NW)
    vmem = functools.partial(pltpu.VMEM, dtype=jnp.float32)
    smem = pl.BlockSpec(memory_space=pltpu.SMEM)
    anywhere = pl.BlockSpec(memory_space=pl.ANY)
    return pl.pallas_call(
        kernel,
        name="reach_avoid",
        out_shape=jax.ShapeDtypeStruct(slab, jnp.float32),
        in_specs=[smem] * 5 + [anywhere] * 3,
        out_specs=anywhere,
        scratch_shapes=[
            vmem((ROW + 1,) + slab),
            vmem((RX + 2, NY + LO + HI, NZ + 16, NW)),
            vmem(slab), vmem(slab), vmem(slab), vmem(slab), vmem(slab), vmem(slab), vmem(slab),
            vmem((NCTRL + 1, G, 8 * ZT, NW)),
            pltpu.SMEM((10 * NCTRL,), jnp.int32),
            pltpu.SMEM((11 * NCTRL,), jnp.float32),
            pltpu.SemaphoreType.DMA((14,)),
            pltpu.SemaphoreType.DMA((8, STAGES + 1)),
            pltpu.SemaphoreType.DMA((len(PARTS),)),
            pltpu.SemaphoreType.DMA((3,)),
            pltpu.SemaphoreType.REGULAR,
        ],
        compiler_params=pltpu.CompilerParams(collective_id=0, has_side_effects=True, vmem_limit_bytes=62 << 20),
    )(fractions.T, control_cost, shard_offset, cell_offset, grid_offset.T, value, target, obstacle)


def solution(mesh):
    grid = P("gx", None, None, None)
    return jax.shard_map(body, mesh=mesh, in_specs=(grid, grid, grid, P(), P(), P(), P(), P()), out_specs=grid,
                         check_vma=False)
```

```python
import functools

import jax
import jax.numpy as jnp
from jax import lax
from jax.experimental import pallas as pl
from jax.experimental.pallas import tpu as pltpu
from jax.sharding import PartitionSpec as P

CX, NY, NZ, NW, NCTRL = 2, 48, 32, 128, 16
ROW = 8
RX = ROW * CX
LO, HI = 4, 5
ENDS = (9, 13, 17, 21, 25, 29, 33, 37, 41, 45, 48)
ORDER = tuple(zip("NNONOHWNOHWNOHWNOHWNOHWNOHWNOHWNWOHNWOHWOHW", (0, 1, 0, 2, 1, 0, 0, 3, 2, 1, 1, 4, 3, 2, 2, 5, 4, 3, 3, 6, 5, 4, 4, 7, 6, 5, 5, 8, 7, 6, 6, 9, 7, 8, 7, 10, 8, 9, 8, 9, 10, 9, 10)))
LAG = 5
LEAD = 1
DEPTH = 2
STAGES = len(ENDS)
CUTS = (0,) + ENDS
OUTS = (0,) + tuple(max(e - LO - HI, 0) for e in ENDS[:-1]) + (NY,)
G, ZT = 4, 2
PARTS = tuple((k, lo, OUTS[k + 1]) for k, lo in enumerate(OUTS[:-2]) if lo < OUTS[k + 1]) + tuple(
    (STAGES - 1, lo, lo + G) for lo in range(OUTS[-2], NY, G))
MESH = pl.DeviceIdType.MESH
SPANS = tuple((ENDS[min(k + LEAD - 1, STAGES - 1)] if k else 0, ENDS[min(k + LEAD, STAGES - 1)]) for k in range(STAGES))
SPANS = (SPANS, tuple(zip(CUTS[:-1], CUTS[1:])))
MOVED = tuple(SPANS[0][k][1] - SPANS[0][k][0] + CUTS[k + 1] - CUTS[k] for k in range(STAGES))
(RIGHT, LEFT, FWD_R, FWD_L, D_OWN, D_L, D_R, D_O, HALO, D_HALO, HALO2, D_HALO2, PART, STORE) = range(14)
(A_RIGHT, A_LEFT, A_FWD, A_D, A_HALO, A_D_HALO, A_HALO2, A_D_HALO2) = range(8)

def kernel(frac, cost, so, co, go, value, target, obstacle, out,
           B, C, P1, Pm, Q1, Qm, A, T, O, R, ip, fp, ssem, rsem, qsem, lsem, ysem):
    n = lax.axis_size("gx")
    me = lax.axis_index("gx")
    j = lax.rem(me, ROW)
    base = me - j
    core = lax.rem(j, 2)
    jr, jl, jo, jp = lax.rem(j + 2, ROW), lax.rem(j + 6, ROW), lax.rem(j + 4, ROW), j + 1 - 2 * core
    qr, ql, qo = jr + 1 - 2 * core, jl + 1 - 2 * core, jo + 1 - 2 * core
    right, left, mate = base + jr, base + jl, base + jp
    up, down = lax.rem(me + ROW, n), lax.rem(me + n - ROW, n)
    last = j == ROW - 1
    beside_last = j == ROW - 2

    loads = [pltpu.make_async_copy(value, B.at[j], lsem.at[0]),
             pltpu.make_async_copy(target, T, lsem.at[1]),
             pltpu.make_async_copy(obstacle, O, lsem.at[2])]
    loads[0].start()

    barrier = pltpu.get_barrier_semaphore()
    for peer in (right, left, mate, down):
        pl.semaphore_signal(barrier, inc=1, device_id=(peer,), device_id_type=MESH)

    loads[0].wait()
    pl.semaphore_wait(barrier, 4)
    pl.semaphore_signal(ysem, inc=1, device_id=(up,), device_id_type=MESH)

    def rank(u, _):
        mine = 2 * so[u] + co[u]
        before = 0
        for v in range(NCTRL):
            other = 2 * so[v] + co[v]
            before += jnp.where((other > mine) | ((other == mine) & (v < u)), 1, 0)
        ip[9 * NCTRL + u] = before
        return 0

    def params(k, _):
        u = 0
        for v in range(NCTRL):
            u += jnp.where(ip[9 * NCTRL + v] == k, v, 0)
        off = 2 * so[u] + co[u]
        for i in range(2):
            q = 2 * j + i + off
            d = jnp.where(q < 0, -1, jnp.where(q < RX, 0, 1))
            before = ip[(6 + i) * NCTRL]
            ip[i * NCTRL + k] = q - RX * d
            fresh = (k == 0) | (d != before)
            fp[(9 + i) * NCTRL + k] = jnp.where(fresh, jnp.inf, -jnp.inf)
            ip[(6 + i) * NCTRL] = d
            for e in (1, 2, 3):
                at = (6 + i) * NCTRL + e
                ip[at] = jnp.where(d == 2 - e, k, jnp.where(k == 0, NCTRL, ip[at]))
        ip[2 * NCTRL + k] = go[0, u]
        ip[3 * NCTRL + k] = go[1, u] + 8
        ip[4 * NCTRL + k] = (NW - go[2, u]) & (NW - 1)
        ip[5 * NCTRL + k] = (NW - 1 - go[2, u]) & (NW - 1)
        f0, f1, f2, f3 = frac[0, u], frac[1, u], frac[2, u], frac[3, u]
        fp[k] = (1.0 - f0) * (1.0 - f2)
        fp[NCTRL + k] = (1.0 - f0) * f2
        fp[2 * NCTRL + k] = f0 * (1.0 - f2)
        fp[3 * NCTRL + k] = f0 * f2
        fp[4 * NCTRL + k] = 1.0 - f1
        fp[5 * NCTRL + k] = f1
        fp[6 * NCTRL + k] = 1.0 - f3
        fp[7 * NCTRL + k] = f3
        fp[8 * NCTRL + k] = cost[u]
        return 0

    def remote(out_sem, in_sem, src, dst, peer):
        return pltpu.make_async_remote_copy(src_ref=src, dst_ref=dst, send_sem=out_sem, recv_sem=in_sem,
                                            device_id=(peer,), device_id_type=MESH)

    def move(kind, arrival, k, peer, slab, rows, to=None):
        for row in rows:
            lo, hi = SPANS[row][k]
            if lo < hi:
                ys = pl.ds(lo, hi - lo)
                remote(ssem.at[kind], rsem.at[arrival, k], B.at[slab, row, ys],
                       B.at[slab if to is None else to, row, ys], peer).start()

    def arrived(arrival, k, peer, cells, slabs=1):
        some = B.at[pl.ds(0, slabs), 0, pl.ds(0, cells)]
        remote(ssem.at[RIGHT], rsem.at[arrival, k], some, some, peer).wait_recv()

    def sent(kind, ref):
        remote(ssem.at[kind], rsem.at[A_RIGHT, 0], ref, ref, right).wait_send()

    def partials(part):
        _, lo, hi = PARTS[part]
        ys = pl.ds(lo, hi - lo)
        for src, dst, peer in ((P1, Q1, down), (Pm, Qm, up)):
            remote(ssem.at[PART], qsem.at[part], src.at[:, ys], dst.at[:, ys], peer).start()

    def fill(k):
        lo, hi = CUTS[k], CUTS[k + 1]

        def put(row, src, y, to):
            C[row, to, pl.ds(0, 8), :] = src[pl.ds(24, 8), :]
            C[row, to, pl.ds(8, 32), :] = src[...]
            C[row, to, pl.ds(40, 8), :] = src[pl.ds(0, 8), :]

        def one(shift, row2):
            def step(y, _):
                rows = (RX + 1,) if row2 else range(RX + 1)
                for row in rows:
                    put(row, B.at[row // 2, row % 2, y], y, y + shift)
                return 0
            return step

        lax.fori_loop(lo, hi, one(0, False), 0)
        if k == 0:
            lax.fori_loop(0, LO + HI, one(NY, False), 0)

        @pl.when(last)
        def _():
            lax.fori_loop(lo, hi, one(0, True), 0)
            if k == 0:
                lax.fori_loop(0, LO + HI, one(NY, True), 0)

    def compute(part):
        _, lo, hi = PARTS[part]

        def tile(t, _):
            i = lax.rem(t, 2)
            t = lax.div(t, 2)
            z = lax.rem(t, NZ // (8 * ZT)) * (8 * ZT)
            y = lo + lax.div(t, NZ // (8 * ZT)) * G

            def control(u, acc):
                row = ip[i * NCTRL + u]
                yy = y + LO + ip[2 * NCTRL + u]
                zz = z + ip[3 * NCTRL + u]
                s1, s2 = ip[4 * NCTRL + u], ip[5 * NCTRL + u]
                f = [fp[q * NCTRL + u] for q in range(8)]
                c, fresh = fp[8 * NCTRL + u], fp[(9 + i) * NCTRL + u]
                fields = []
                for q in range(G + 1):
                    low = f[0] * C[row, yy + q, pl.ds(zz, 8 * ZT), :] + f[1] * C[row, yy + q, pl.ds(zz + 1, 8 * ZT), :]
                    high = f[2] * C[row + 1, yy + q, pl.ds(zz, 8 * ZT), :] + f[3] * C[row + 1, yy + q, pl.ds(zz + 1, 8 * ZT), :]
                    fields.append(low + high)
                new = []
                for q in range(G):
                    h = f[4] * fields[q] + f[5] * fields[q + 1]
                    w = f[6] * pltpu.roll(h, s1, 1) + f[7] * pltpu.roll(h, s2, 1)
                    new.append(jnp.minimum(jnp.maximum(acc[q], fresh), w + c))
                    R[u, q] = new[q]
                return tuple(new)

            start = tuple([jnp.full((8 * ZT, NW), jnp.inf, jnp.float32)] * G)
            lax.fori_loop(0, NCTRL, control, start, unroll=True)
            zs = pl.ds(pl.multiple_of(z, 8), 8 * ZT)
            for q in range(G):
                for e, ref in ((1, P1), (2, A), (3, Pm)):
                    ref[i, y + q, zs, :] = R[ip[(6 + i) * NCTRL + e], q]
            return 0

        lax.fori_loop(0, 2 * ((hi - lo) // G) * (NZ // (8 * ZT)), tile, 0)

    def combine(part):
        _, lo, hi = PARTS[part]
        some = Q1.at[:, pl.ds(0, 2 * (hi - lo))]
        remote(ssem.at[PART], qsem.at[part], some, some, down).wait_recv()

        def step(y, _):
            at = lax.rem(y + LO, NY)
            for i in range(2):
                best = jnp.minimum(A[i, y], jnp.minimum(Q1[i, y], Qm[i, y]))
                A[i, y] = jnp.maximum(O[i, at], jnp.minimum(T[i, at], best))
            return 0

        lax.fori_loop(lo, hi, step, 0)

    def own(k):
        if k < STAGES:
            move(RIGHT, A_RIGHT, k, right, j, (0, 1))
            move(LEFT, A_LEFT, k, left, j, (0, 1))

    def halo(k, which):
        @pl.when(which)
        def _():
            move(HALO, A_HALO, k, down, 0, (0,), ROW)

    def neighbours(k):
        arrived(A_RIGHT, k, right, MOVED[k])
        move(FWD_R, A_FWD, k, right, jl, (0,))
        move(D_L, A_D, k, mate, jl, (0, 1))
        if k == 0:
            pl.semaphore_wait(ysem, 1)
            for early in range(STAGES):
                halo(early, j == 0)
        halo(k, j == 2)
        arrived(A_LEFT, k, left, MOVED[k])
        move(FWD_L, A_FWD, k, left, jr, (1,))
        move(D_R, A_D, k, mate, jr, (0, 1))
        halo(k, beside_last)

        @pl.when(beside_last)
        def _():
            move(HALO2, A_HALO2, k, down, 0, (1,), ROW)

        own(k + DEPTH)

    def opposite(k):
        arrived(A_FWD, k, right, MOVED[k])
        halo(k, j == 4)
        move(D_O, A_D, k, mate, jo, (0, 1))

    def pass_halo(k):
        @pl.when(core == 0)
        def _():
            arrived(A_HALO, k, down, SPANS[0][k][1] - SPANS[0][k][0])
            move(D_HALO, A_D_HALO, k, mate, ROW, (0,))

    def work(k):
        @pl.when(beside_last)
        def _():
            arrived(A_HALO2, k, down, CUTS[k + 1] - CUTS[k])
            move(D_HALO2, A_D_HALO2, k, mate, ROW, (1,))

        if k == 0:
            remote(ssem.at[D_OWN], rsem.at[A_D, STAGES], B.at[jp], B.at[jp], mate).wait_recv()
        arrived(A_D, k, mate, MOVED[k], 3)
        if k == 0 or k > LEAD:
            ahead = max(k - LEAD, 0)

            @pl.when(core == 1)
            def _():
                arrived(A_D_HALO, ahead, mate, SPANS[0][ahead][1] - SPANS[0][ahead][0])

        @pl.when(last)
        def _():
            arrived(A_D_HALO2, k, mate, CUTS[k + 1] - CUTS[k])

        fill(k)
        for part, (stage, _, _) in enumerate(PARTS):
            if stage == k:
                compute(part)
                partials(part)

    def store(part):
        _, lo, hi = PARTS[part]
        return pltpu.make_async_copy(A.at[:, pl.ds(lo, hi - lo)], out.at[:, pl.ds((lo + LO) % NY, hi - lo)],
                                     ssem.at[STORE])

    def finish(stage):
        for part, (k, _, _) in enumerate(PARTS):
            if k == stage:
                combine(part)
                store(part).start()

    def drain():
        for kind, ref in ((RIGHT, B.at[j]), (LEFT, B.at[j]), (FWD_R, B.at[jl, 0]), (FWD_L, B.at[jr, 1]), (D_OWN, B.at[j]),
                          (D_L, B.at[jl]), (D_R, B.at[jr]), (D_O, B.at[jo])):
            sent(kind, ref)

        @pl.when(core == 0)
        def _():
            sent(HALO, B.at[0, 0])
            sent(D_HALO, B.at[ROW, 0])

        @pl.when(beside_last)
        def _():
            sent(HALO2, B.at[0, 1])
            sent(D_HALO2, B.at[ROW, 1])

    for k in range(DEPTH):
        own(k)
    remote(ssem.at[D_OWN], rsem.at[A_D, STAGES], B.at[j], B.at[j], mate).start()
    loads[1].start()
    loads[2].start()
    R[NCTRL] = jnp.full(R.shape[1:], jnp.inf, jnp.float32)
    for i in range(2):
        ip[(6 + i) * NCTRL] = 0
        for e in (1, 2, 3):
            ip[(6 + i) * NCTRL + e] = 0
    lax.fori_loop(0, NCTRL, rank, 0)
    lax.fori_loop(0, NCTRL, params, 0)
    for what, k in ORDER:
        if what == "N":
            neighbours(k)
        elif what == "O":
            opposite(k)
        elif what == "H":
            pass_halo(k)
        else:
            work(k)
            if k == 1:
                loads[1].wait()
                loads[2].wait()
            if k >= LAG:
                finish(k - LAG)
    drain()
    for k in range(STAGES - LAG, STAGES):
        finish(k)

    sent(PART, B.at[pl.ds(0, 2)])
    pltpu.make_async_copy(A, out, ssem.at[STORE]).wait()


def body(value, target, obstacle, fractions, control_cost, shard_offset, cell_offset, grid_offset):
    slab = (CX, NY, NZ, NW)
    vmem = functools.partial(pltpu.VMEM, dtype=jnp.float32)
    smem = pl.BlockSpec(memory_space=pltpu.SMEM)
    anywhere = pl.BlockSpec(memory_space=pl.ANY)
    return pl.pallas_call(
        kernel,
        name="reach_avoid",
        out_shape=jax.ShapeDtypeStruct(slab, jnp.float32),
        in_specs=[smem] * 5 + [anywhere] * 3,
        out_specs=anywhere,
        scratch_shapes=[
            vmem((ROW + 1,) + slab),
            vmem((RX + 2, NY + LO + HI, NZ + 16, NW)),
            vmem(slab), vmem(slab), vmem(slab), vmem(slab), vmem(slab), vmem(slab), vmem(slab),
            vmem((NCTRL + 1, G, 8 * ZT, NW)),
            pltpu.SMEM((10 * NCTRL,), jnp.int32),
            pltpu.SMEM((11 * NCTRL,), jnp.float32),
            pltpu.SemaphoreType.DMA((14,)),
            pltpu.SemaphoreType.DMA((8, STAGES + 1)),
            pltpu.SemaphoreType.DMA((len(PARTS),)),
            pltpu.SemaphoreType.DMA((3,)),
            pltpu.SemaphoreType.REGULAR,
        ],
        compiler_params=pltpu.CompilerParams(collective_id=0, has_side_effects=True, vmem_limit_bytes=62 << 20),
    )(fractions.T, control_cost, shard_offset, cell_offset, grid_offset.T, value, target, obstacle)


def solution(mesh):
    grid = P("gx", None, None, None)
    return jax.shard_map(body, mesh=mesh, in_specs=(grid, grid, grid, P(), P(), P(), P(), P()), out_specs=grid,
                         check_vma=False)
```
